32 devices in a mesh: rep: 2 (over z, core), dp: 16 (over x, y).
Axes of the slice: x: 4, y: 4, z: 1, core: 2. Of those that a mesh axis runs over, the one named last changes fastest.
The devices are a block of a 4x4x8 slice.
Arguments:
- g_w_gate: bfloat16 [32, 2, 768, 3072], P(('rep', 'dp')), parts along dimension 0
- g_w_up: bfloat16 [32, 2, 768, 3072], P(('rep', 'dp')), parts along dimension 0
- g_w_down: bfloat16 [32, 2, 3072, 768], P(('rep', 'dp')), parts along dimension 0
- w_gate: bfloat16 [2, 768, 3072], replicated
- w_up: bfloat16 [2, 768, 3072], replicated
- w_down: bfloat16 [2, 3072, 768], replicated
- m_w_gate: float32 [2, 768, 3072], P(None, 'dp')
- m_w_up: float32 [2, 768, 3072], P(None, 'dp')
- m_w_down: float32 [2, 3072, 768], P(None, 'dp')
- v_w_gate: float32 [2, 768, 3072], P(None, 'dp')
- v_w_up: float32 [2, 768, 3072], P(None, 'dp')
- v_w_down: float32 [2, 3072, 768], P(None, 'dp')
Outputs:
- output 1: bfloat16 [4, 768, 3072], P('rep'), parts along dimension 0
- output 2: bfloat16 [4, 768, 3072], P('rep'), parts along dimension 0
- output 3: bfloat16 [4, 3072, 768], P('rep'), parts along dimension 0
- output 4: float32 [4, 768, 3072], P('rep', 'dp'), parts along dimension 0
- output 5: float32 [4, 768, 3072], P('rep', 'dp'), parts along dimension 0
- output 6: float32 [4, 3072, 768], P('rep', 'dp'), parts along dimension 0
- output 7: float32 [4, 768, 3072], P('rep', 'dp'), parts along dimension 0
- output 8: float32 [4, 768, 3072], P('rep', 'dp'), parts along dimension 0
- output 9: float32 [4, 3072, 768], P('rep', 'dp'), parts along dimension 0
There are 2 independent parts. The reference program is written for one: setup_inputs(seed, part) draws one part's arguments, and reference() takes and returns one part's arrays. A program takes and returns all parts, laid end to end along the dimension named above; an argument that names none is the same for every part.
All inputs are finite; a program needn't handle non-finite values.
Results may differ from the reference program's by a relative error of at most 0.022.
Values are sent between devices in bfloat16 or wider.
A program may use at most 768 MiB of HBM per device.

```python
import jax
import jax.numpy as jnp
from jax import lax

DEVICES = 16
D = 768
FF = 3072
LAYERS = 2
NAMES = ("w_gate", "w_up", "w_down")
SHAPES = {"w_gate": (LAYERS, D, FF), "w_up": (LAYERS, D, FF), "w_down": (LAYERS, FF, D)}


def setup_inputs(seed: int = 0, part: int = 0) -> dict:
    kz, *keys = jax.random.split(jax.random.key(seed), 1 + 5 * len(NAMES))
    loud = 2.0 ** jax.random.uniform(kz, (), jnp.float32, -1.0, 1.0)
    drawn = {}
    for name, key, both in zip(NAMES, keys[:3], keys[3:6], strict=True):
        own = jax.random.normal(jax.random.fold_in(key, part), (DEVICES, *SHAPES[name]), jnp.float32)
        shared = jax.random.normal(jax.random.fold_in(both, part), SHAPES[name], jnp.float32)
        drawn["g_" + name] = (loud * (0.7 * shared / DEVICES + 0.7 * own * DEVICES**-0.5)).astype(jnp.bfloat16)
    for name, key in zip(NAMES, keys[6:9], strict=True):
        drawn[name] = (jax.random.normal(key, SHAPES[name], jnp.float32) * SHAPES[name][1] ** -0.5).astype(jnp.bfloat16)
    for name, key in zip(NAMES, keys[9:12], strict=True):
        drawn["m_" + name] = loud * 0.5 * jax.random.normal(key, SHAPES[name], jnp.float32)
    for name, key in zip(NAMES, keys[12:15], strict=True):
        drawn["v_" + name] = loud * loud * jax.random.uniform(key, SHAPES[name], jnp.float32, 0.5, 1.5)
    return drawn


def adamw(w, m, v, g):
    m = 0.9 * m + 0.1 * g
    v = 0.95 * v + 0.05 * g * g
    step = m * lax.rsqrt(v + 1e-8) + 0.1 * w
    return (w - 0.02 * step).astype(jnp.bfloat16), m, v


def clipped(gradients, sum_of_squares, count):
    factor = jnp.minimum(1.0, 0.5 * lax.rsqrt(sum_of_squares / count + 1e-30))
    return [g * factor for g in gradients]


def reference(g_w_gate, g_w_up, g_w_down, w_gate, w_up, w_down, m_w_gate, m_w_up, m_w_down, v_w_gate, v_w_up, v_w_down):
    def total(terms):
        return lax.scan(lambda so_far, term: (so_far + term.astype(jnp.float32), None), jnp.zeros(terms.shape[1:], jnp.float32), terms)[0]

    gradients = [total(terms).astype(jnp.bfloat16).astype(jnp.float32) for terms in (g_w_gate, g_w_up, g_w_down)]
    gradients = clipped(gradients, sum(jnp.sum(g * g) for g in gradients), sum(g.size for g in gradients))
    new = [
        adamw(w.astype(jnp.float32), m, v, g)
        for w, m, v, g in zip((w_gate, w_up, w_down), (m_w_gate, m_w_up, m_w_down), (v_w_gate, v_w_up, v_w_down), gradients, strict=True)
    ]
    return tuple(one[which] for which in range(3) for one in new)
```

```python
import functools
import heapq
import math

import jax
import jax.numpy as jnp
from jax import lax
from jax.experimental import pallas as pl
from jax.experimental.pallas import tpu as pltpu
from jax.sharding import PartitionSpec as P

MESH = pl.DeviceIdType.MESH
F32 = jnp.float32
PARTS = (0, 1)
HALVES = (0, 1)
RINGS = 5
SLAB_SENDS = 6


def gather_sends(part, ring):
    axis = 1 - part if ring == 0 else part
    return [(0, 1, 0, axis), (1, -1, 1, axis), (2, 1, 1, axis), (3, -1, 0, axis), (4, 1, 0, axis), (5, -1, 1, axis)]


def gather_next(arrays_and_parts):
    follow = {}
    for a, p in arrays_and_parts:
        for kind, k, half in ((0, 3, 0), (1, 1, 1), (2, 3, 1), (3, 1, 0), (4, 2, 0), (5, 2, 1)):
            relay = [(a, p, 0, 4 + kind)] if kind < 2 else []
            follow[a, p, 0, kind] = relay + [(a, p, 1 + k, 0 if half == 0 else 1), (a, p, 1 + k, 3 if half == 0 else 2)]
        for k in range(4):
            for kind in range(SLAB_SENDS):
                follow[a, p, 1 + k, kind] = [(a, p, 1 + k, 4 + kind)] if kind < 2 else []
    free = {}
    arrivals = []
    order = []

    def put(send, now):
        a, p, ring, kind = send
        _, direction, _, axis = gather_sends(p, ring)[kind]
        start = max(now, free.get((axis, direction), 0.0))
        free[axis, direction] = start + 3.2
        heapq.heappush(arrivals, (start + 3.2 + 2.0, len(order) + len(arrivals), send))

    for i, (a, p) in enumerate(arrays_and_parts):
        for ring in (0, 1):
            for kind in range(4):
                put((a, p, ring, kind), 0.4 * i)
    while arrivals:
        now, _, send = heapq.heappop(arrivals)
        order.append((send, follow[send]))
        for one in follow[send]:
            put(one, now)
    return order


def kernel(side, count, *refs):
    terms, weights, m_in, v_in, whole, m_out, v_out = (refs[3 * i : 3 * i + 3] for i in range(7))
    own, weight = refs[21:24], refs[24:27]
    squares, load_sem, send_sem, recv_sem, gsend_sem, grecv_sem, nsend_sem, nrecv_sem = refs[27:]
    arrays = range(3)
    me = lax.axis_index("dp")
    at = (me // side, me % side)

    def device(axis, by):
        moved = lax.rem(at[axis] + by + side, side)
        return {"dp": moved * side + at[1] if axis == 0 else at[0] * side + moved}

    def place(axis, by):
        return lax.rem(at[axis] + by + side, side)

    def columns(a, half):
        wide = terms[a].shape[-1] // 2
        return pl.ds(half * wide, wide)

    def row_blocks(a):
        rows = terms[a].shape[-2]
        return 3 if rows % 48 == 0 else 1

    def load(a, p, which):
        if which == 0:
            t = place(p, 0)
            source = terms[a].at[0, p, t] if p == 0 else terms[a].at[0, p, :, t]
            return pltpu.make_async_copy(source, own[a].at[p, 0], load_sem.at[a, p, 0])
        half = which - 1
        t = place(p, 1 if half == 0 else -1)
        cols = columns(a, half)
        source = terms[a].at[0, p, t, :, :, cols] if p == 0 else terms[a].at[0, p, :, t, :, cols]
        return pltpu.make_async_copy(source, own[a].at[p, 1, :, :, cols], load_sem.at[a, p, which])

    def load_state(a, which):
        if which == 0:
            return pltpu.make_async_copy(weights[a].at[:, at[0], at[1]], weight[a], load_sem.at[a, 0, 3])
        if which == 1:
            return pltpu.make_async_copy(m_in[a], m_out[a], load_sem.at[a, 1, 3])
        return pltpu.make_async_copy(v_in[a], v_out[a], load_sem.at[a, 0, 4])

    for a in arrays:
        for p in PARTS:
            for half in HALVES:
                load(a, p, 1 + half).start()

    barrier = pltpu.get_barrier_semaphore()
    for by in range(1, side * side):
        pl.semaphore_signal(barrier, inc=1, device_id={"dp": lax.rem(me + by, side * side)}, device_id_type=MESH)
    pl.semaphore_wait(barrier, side * side - 1)

    def first(a, p, half, kind):
        up = 1 if half == 0 else -1
        cols = columns(a, half)
        if kind == 2:
            source, by = own[a].at[p, 1, :, :, cols], up
        else:
            by = up if kind == 0 else -up
            t = place(p, 2 if kind == 0 else by)
            source = terms[a].at[0, p, t, :, :, cols] if p == 0 else terms[a].at[0, p, :, t, :, cols]
        return pltpu.make_async_remote_copy(
            src_ref=source,
            dst_ref=whole[a].at[p, kind, :, :, cols],
            send_sem=send_sem.at[a, p, half, kind],
            recv_sem=recv_sem.at[a, p, half, kind],
            device_id=device(p, by),
            device_id_type=MESH,
        )

    def second(a, p, half, kind):
        up = 1 if half == 0 else -1
        cols = columns(a, half)
        by = -up if kind == 1 else up
        j = place(1 - p, 2 if kind == 0 else by)
        return pltpu.make_async_remote_copy(
            src_ref=own[a].at[p, 0, j, :, cols],
            dst_ref=whole[a].at[p, 3, kind, :, cols],
            send_sem=send_sem.at[a, p, half, 3 + kind],
            recv_sem=recv_sem.at[a, p, half, 3 + kind],
            device_id=device(1 - p, by),
            device_id_type=MESH,
        )

    def rows_of(a, i):
        rows = terms[a].shape[-2] // row_blocks(a)
        return pl.ds(pl.multiple_of(i * rows, rows), rows)

    def add(a, p, half, j, extra):
        cols = columns(a, half)

        def body(i, carry):
            rows = rows_of(a, i)
            total = own[a][p, 0, j, rows, cols].astype(F32)
            for k in (1, 2):
                total += whole[a][p, k, j, rows, cols].astype(F32)
            for k in extra:
                total += whole[a][p, 3, k, rows, cols].astype(F32)
            total = total.astype(jnp.bfloat16)
            own[a][p, 0, j, rows, cols] = total
            if carry is None:
                return None
            total = total.astype(F32)
            total = total * total
            total = sum(total[:, c : c + 128] for c in range(0, total.shape[1], 128))
            return carry + sum(total[r : r + 8] for r in range(0, total.shape[0], 8))

        return body

    every = [(p, half) for p in PARTS for half in HALVES]
    for a in arrays:
        for p, half in every:
            first(a, p, half, 0).start()
    for a in arrays:
        for p in PARTS:
            load(a, p, 0).start()
    for a in arrays:
        for which in range(3):
            load_state(a, which).start()
    for a in arrays:
        for p, half in every:
            first(a, p, half, 1).start()
            load(a, p, 1 + half).wait()
            first(a, p, half, 0).wait_recv()
            cols = columns(a, half)
            blocks = row_blocks(a)

            def relay(i, _, a=a, p=p, cols=cols, blocks=blocks):
                j, rows = i // blocks, rows_of(a, i % blocks)
                total = own[a][p, 1, j, rows, cols].astype(F32) + whole[a][p, 0, j, rows, cols].astype(F32)
                own[a][p, 1, j, rows, cols] = total.astype(jnp.bfloat16)

            lax.fori_loop(0, side * blocks, relay, None)
            first(a, p, half, 2).start()
    for a in arrays:
        for p in PARTS:
            load(a, p, 0).wait()
        for p, half in every:
            up = 1 if half == 0 else -1
            first(a, p, half, 1).wait_recv()
            first(a, p, half, 2).wait_recv()
            for kind in (0, 1):
                j = place(1 - p, 2 if kind == 0 else -up)
                lax.fori_loop(0, row_blocks(a), lambda i, c, f=add(a, p, half, j, ()): f(i, c), None)
                second(a, p, half, kind).start()
    for a in arrays:
        for p, half in every:
            up = 1 if half == 0 else -1
            second(a, p, half, 0).wait_recv()
            lax.fori_loop(0, row_blocks(a), lambda i, c, f=add(a, p, half, place(1 - p, up), (0,)): f(i, c), None)
            second(a, p, half, 2).start()
    total = jnp.zeros((8, 128), F32)
    for a in arrays:
        for p, half in every:
            second(a, p, half, 1).wait_recv()
            second(a, p, half, 2).wait_recv()
            total = lax.fori_loop(0, row_blocks(a), add(a, p, half, at[1 - p], (1, 2)), total)

    squares[me] = total

    def tell(by):
        return pltpu.make_async_remote_copy(
            src_ref=squares.at[me],
            dst_ref=squares.at[me],
            send_sem=nsend_sem.at[by - 1],
            recv_sem=nrecv_sem.at[by - 1],
            device_id={"dp": lax.rem(me + by, side * side)},
            device_id_type=MESH,
        )

    for by in range(1, side * side):
        tell(by).start()
    for a in arrays:
        for which in range(3):
            load_state(a, which).wait()
        for p, half in every:
            for kind in range(3):
                first(a, p, half, kind).wait_send()
                second(a, p, half, kind).wait_send()
    for by in range(1, side * side):
        tell(by).wait_recv()
    total = squares[0]
    for i in range(1, side * side):
        total += squares[i]
    total = jnp.sum(jnp.sum(total, axis=1, keepdims=True), axis=0, keepdims=True)
    factor = jnp.minimum(1.0, 0.5 * lax.rsqrt(total / count + 1e-30))

    def send(a, p, ring, kind):
        _, direction, half, axis = gather_sends(p, ring)[kind]
        cols = columns(a, half)
        back = direction if kind >= 4 else 0
        along = place(axis, -back)
        if ring == 0:
            other = at[1 - axis]
        else:
            other = place(1 - axis, ring - 1)
        block = whole[a].at[p, along, other, :, cols] if axis == 0 else whole[a].at[p, other, along, :, cols]
        return pltpu.make_async_remote_copy(
            src_ref=block,
            dst_ref=block,
            send_sem=gsend_sem.at[a, p, ring, kind],
            recv_sem=grecv_sem.at[a, p, ring, kind],
            device_id=device(axis, direction),
            device_id_type=MESH,
        )

    slabs = [(a, p) for a in arrays for p in PARTS]
    for a, p in slabs:
        for half in HALVES:
            cols = columns(a, half)

            def update(i, _, a=a, p=p, cols=cols):
                rows = rows_of(a, i)
                g = own[a][p, 0, at[1 - p], rows, cols].astype(F32) * factor
                w = weight[a][p, rows, cols].astype(F32)
                m = 0.9 * m_out[a][p, rows, cols] + 0.1 * g
                v = 0.95 * v_out[a][p, rows, cols] + 0.05 * g * g
                m_out[a][p, rows, cols] = m
                v_out[a][p, rows, cols] = v
                step = m * lax.rsqrt(v + 1e-8) + 0.1 * w
                whole[a][p, at[0], at[1], rows, cols] = (w - 0.02 * step).astype(jnp.bfloat16)

            lax.fori_loop(0, row_blocks(a), update, None)
        for ring in (0, 1):
            for kind in range(4):
                send(a, p, ring, kind).start()
    for one, then in gather_next(slabs):
        send(*one).wait_recv()
        for other in then:
            send(*other).start()
    for a, p in slabs:
        for ring in range(RINGS):
            for kind in range(SLAB_SENDS):
                send(a, p, ring, kind).wait_send()
    for by in range(1, side * side):
        tell(by).wait_send()


def store(*refs):
    here, there, sem = refs[:9], refs[9:18], refs[18]
    copies = [pltpu.make_async_copy(a, b, sem.at[i]) for i, (a, b) in enumerate(zip(here, there, strict=True))]
    for copy in copies:
        copy.start()
    for copy in copies:
        copy.wait()


def solution(mesh):
    devices = mesh.shape["dp"]
    side = math.isqrt(devices)

    def step(*arrays):
        terms, weights, m, v = (arrays[i : i + 3] for i in (0, 3, 6, 9))

        def blocks(x):
            return x.reshape(*x.shape[:-2], side, side, x.shape[-2] // devices, x.shape[-1])

        shapes = [one.shape for one in m]
        wholes = [blocks(w).shape for w in weights]
        count = devices * sum(math.prod(s) for s in shapes)
        out = pl.pallas_call(
            functools.partial(kernel, side, count),
            out_shape=[pltpu.VMEM(s, jnp.bfloat16) for s in wholes] + [pltpu.VMEM(s, F32) for s in shapes * 2],
            in_specs=[pl.BlockSpec(memory_space=pltpu.HBM)] * 12,
            out_specs=[pl.BlockSpec(memory_space=pltpu.VMEM)] * 9,
            scratch_shapes=[pltpu.VMEM((2, 2, side, *s[1:]), jnp.bfloat16) for s in shapes]
            + [pltpu.VMEM(s, jnp.bfloat16) for s in shapes]
            + [
                pltpu.VMEM((devices, 8, 128), F32),
                pltpu.SemaphoreType.DMA((3, 2, 5)),
                pltpu.SemaphoreType.DMA((3, 2, 2, 6)),
                pltpu.SemaphoreType.DMA((3, 2, 2, 6)),
                pltpu.SemaphoreType.DMA((3, 2, RINGS, SLAB_SENDS)),
                pltpu.SemaphoreType.DMA((3, 2, RINGS, SLAB_SENDS)),
                pltpu.SemaphoreType.DMA((devices - 1,)),
                pltpu.SemaphoreType.DMA((devices - 1,)),
            ],
            compiler_params=pltpu.CompilerParams(collective_id=0, has_side_effects=True, vmem_limit_bytes=20 * 2**20),
        )(*(blocks(t) for t in terms), *(blocks(w) for w in weights), *m, *v)
        out = pl.pallas_call(
            store,
            out_shape=[jax.ShapeDtypeStruct(o.shape, o.dtype) for o in out],
            in_specs=[pl.BlockSpec(memory_space=pltpu.VMEM)] * 9,
            out_specs=[pl.BlockSpec(memory_space=pltpu.HBM)] * 9,
            scratch_shapes=[pltpu.SemaphoreType.DMA((9,))],
            compiler_params=pltpu.CompilerParams(vmem_limit_bytes=2**20),
        )(*(pltpu.with_memory_space_constraint(o, pltpu.VMEM) for o in out))
        return (*(o.reshape(w.shape) for o, w in zip(out[:3], weights, strict=True)), *out[3:])

    all_of, cut = P(None, None, None), P(None, "dp", None)
    return jax.shard_map(
        step,
        mesh=mesh,
        in_specs=(P(("rep", "dp"), None, None, None),) * 3 + (all_of,) * 3 + (cut,) * 6,
        out_specs=(P("rep", None, None),) * 3 + (P("rep", "dp", None),) * 6,
        check_vma=False,
    )
```

```python
import functools
import heapq
import math

import jax
import jax.numpy as jnp
from jax import lax
from jax.experimental import pallas as pl
from jax.experimental.pallas import tpu as pltpu
from jax.sharding import PartitionSpec as P

MESH = pl.DeviceIdType.MESH
F32 = jnp.float32
PARTS = (0, 1)
HALVES = (0, 1)
RINGS = 5
KINDS = 6


def gather_kinds(ring):
    relays = {4: (1, 0, True), 5: (-1, 1, True)}
    if ring == 3:
        return {0: (1, 0, False), 1: (-1, 1, False), 2: (1, 1, False), 3: (-1, 0, False), **relays}
    return {0: (1, None, False), 1: (-1, None, False), **relays}


def gather_order(slabs):
    follow = {}
    for a, p in slabs:
        for ring in range(RINGS):
            for kind, (_, _, relayed) in gather_kinds(ring).items():
                follow[a, p, ring, kind] = [(a, p, ring, 4 + kind)] if kind < 2 else []
        for kind, k in ((0, 3), (1, 1)):
            follow[a, p, 0, kind] += [(a, p, 1 + k, 0), (a, p, 1 + k, 1)]
        follow[a, p, 0, 4] += [(a, p, 3, 0), (a, p, 3, 3)]
        follow[a, p, 0, 5] += [(a, p, 3, 1), (a, p, 3, 2)]
    free, arrivals, order, made = {}, [], [], 0

    def put(send, now):
        nonlocal made
        a, p, ring, kind = send
        direction, half, _ = gather_kinds(ring)[kind]
        way = (1 - p if ring == 0 else p, direction)
        free[way] = max(now, free.get(way, 0.0)) + (6.4 if half is None else 3.2)
        made += 1
        heapq.heappush(arrivals, (free[way] + 2.0, made, send))

    for i, (a, p) in enumerate(slabs):
        for ring in (0, 1):
            for kind in (0, 1):
                put((a, p, ring, kind), 0.4 * i)
    while arrivals:
        now, _, send = heapq.heappop(arrivals)
        order.append((send, follow[send]))
        for one in follow[send]:
            put(one, now)
    return order


def kernel(side, count, *refs):
    terms, weights, m_in, v_in, whole, m_out, v_out = (refs[3 * i : 3 * i + 3] for i in range(7))
    own, weight = refs[21:24], refs[24:27]
    squares, load_sem, send_sem, recv_sem, gsend_sem, grecv_sem, nsend_sem, nrecv_sem = refs[27:]
    arrays = range(3)
    me = lax.axis_index("dp")
    at = (me // side, me % side)

    def device(axis, by):
        moved = lax.rem(at[axis] + by + side, side)
        return {"dp": moved * side + at[1] if axis == 0 else at[0] * side + moved}

    def place(axis, by):
        return lax.rem(at[axis] + by + side, side)

    def columns(a, half):
        wide = terms[a].shape[-1] // 2
        return pl.ds(half * wide, wide)

    def row_blocks(a):
        rows = terms[a].shape[-2]
        return 3 if rows % 48 == 0 else 1

    def load(a, p, which):
        if which == 0:
            t = place(p, 0)
            source = terms[a].at[0, p, t] if p == 0 else terms[a].at[0, p, :, t]
            return pltpu.make_async_copy(source, own[a].at[p, 0], load_sem.at[a, p, 0])
        half = which - 1
        t = place(p, 1 if half == 0 else -1)
        cols = columns(a, half)
        source = terms[a].at[0, p, t, :, :, cols] if p == 0 else terms[a].at[0, p, :, t, :, cols]
        return pltpu.make_async_copy(source, own[a].at[p, 1, :, :, cols], load_sem.at[a, p, which])

    def load_state(a, which):
        if which == 0:
            return pltpu.make_async_copy(weights[a].at[:, at[0], at[1]], weight[a], load_sem.at[a, 0, 3])
        if which == 1:
            return pltpu.make_async_copy(m_in[a], m_out[a], load_sem.at[a, 1, 3])
        return pltpu.make_async_copy(v_in[a], v_out[a], load_sem.at[a, 0, 4])

    for a in arrays:
        for p in PARTS:
            for half in HALVES:
                load(a, p, 1 + half).start()

    barrier = pltpu.get_barrier_semaphore()
    for axis in (0, 1):
        for by in (1, -1):
            pl.semaphore_signal(barrier, inc=1, device_id=device(axis, by), device_id_type=MESH)
    pl.semaphore_wait(barrier, 4)

    def first(a, p, half, kind):
        up = 1 if half == 0 else -1
        cols = columns(a, half)
        if kind == 2:
            source, by = own[a].at[p, 1, :, :, cols], up
        else:
            by = up if kind == 0 else -up
            t = place(p, 2 if kind == 0 else by)
            source = terms[a].at[0, p, t, :, :, cols] if p == 0 else terms[a].at[0, p, :, t, :, cols]
        return pltpu.make_async_remote_copy(
            src_ref=source,
            dst_ref=whole[a].at[p, kind, :, :, cols],
            send_sem=send_sem.at[a, p, half, kind],
            recv_sem=recv_sem.at[a, p, half, kind],
            device_id=device(p, by),
            device_id_type=MESH,
        )

    def second(a, p, half, kind):
        up = 1 if half == 0 else -1
        cols = columns(a, half)
        by = -up if kind == 1 else up
        j = place(1 - p, 2 if kind == 0 else by)
        return pltpu.make_async_remote_copy(
            src_ref=own[a].at[p, 0, j, :, cols],
            dst_ref=whole[a].at[p, 3, kind, :, cols],
            send_sem=send_sem.at[a, p, half, 3 + kind],
            recv_sem=recv_sem.at[a, p, half, 3 + kind],
            device_id=device(1 - p, by),
            device_id_type=MESH,
        )

    def rows_of(a, i):
        rows = terms[a].shape[-2] // row_blocks(a)
        return pl.ds(pl.multiple_of(i * rows, rows), rows)

    def add(a, p, half, j, extra):
        cols = columns(a, half)

        def body(i, carry):
            rows = rows_of(a, i)
            total = own[a][p, 0, j, rows, cols].astype(F32)
            for k in (1, 2):
                total += whole[a][p, k, j, rows, cols].astype(F32)
            for k in extra:
                total += whole[a][p, 3, k, rows, cols].astype(F32)
            total = total.astype(jnp.bfloat16)
            own[a][p, 0, j, rows, cols] = total
            if carry is None:
                return None
            total = total.astype(F32)
            total = total * total
            total = sum(total[:, c : c + 128] for c in range(0, total.shape[1], 128))
            return carry + sum(total[r : r + 8] for r in range(0, total.shape[0], 8))

        return body

    every = [(p, half) for p in PARTS for half in HALVES]
    for a in arrays:
        for p, half in every:
            first(a, p, half, 0).start()
    for a in arrays:
        for p in PARTS:
            load(a, p, 0).start()
    for a in arrays:
        for which in range(3):
            load_state(a, which).start()
    for a in arrays:
        for p, half in every:
            first(a, p, half, 1).start()
            load(a, p, 1 + half).wait()
            first(a, p, half, 0).wait_recv()
            cols = columns(a, half)
            blocks = row_blocks(a)

            def relay(i, _, a=a, p=p, cols=cols, blocks=blocks):
                j, rows = i // blocks, rows_of(a, i % blocks)
                total = own[a][p, 1, j, rows, cols].astype(F32) + whole[a][p, 0, j, rows, cols].astype(F32)
                own[a][p, 1, j, rows, cols] = total.astype(jnp.bfloat16)

            lax.fori_loop(0, side * blocks, relay, None)
            first(a, p, half, 2).start()
    for a in arrays:
        for p in PARTS:
            load(a, p, 0).wait()
        for p, half in every:
            up = 1 if half == 0 else -1
            first(a, p, half, 1).wait_recv()
            first(a, p, half, 2).wait_recv()
            for kind in (0, 1):
                j = place(1 - p, 2 if kind == 0 else -up)
                lax.fori_loop(0, row_blocks(a), lambda i, c, f=add(a, p, half, j, ()): f(i, c), None)
                second(a, p, half, kind).start()
    for a in arrays:
        for p, half in every:
            up = 1 if half == 0 else -1
            second(a, p, half, 0).wait_recv()
            lax.fori_loop(0, row_blocks(a), lambda i, c, f=add(a, p, half, place(1 - p, up), (0,)): f(i, c), None)
            second(a, p, half, 2).start()
    total = jnp.zeros((8, 128), F32)
    for a in arrays:
        for p, half in every:
            second(a, p, half, 1).wait_recv()
            second(a, p, half, 2).wait_recv()
            total = lax.fori_loop(0, row_blocks(a), add(a, p, half, at[1 - p], (1, 2)), total)

    squares[me] = total

    def tell(by):
        return pltpu.make_async_remote_copy(
            src_ref=squares.at[me],
            dst_ref=squares.at[me],
            send_sem=nsend_sem.at[by - 1],
            recv_sem=nrecv_sem.at[by - 1],
            device_id={"dp": lax.rem(me + by, side * side)},
            device_id_type=MESH,
        )

    for by in range(1, side * side):
        tell(by).start()
    for a in arrays:
        for which in range(3):
            load_state(a, which).wait()
        for p, half in every:
            for kind in range(3):
                first(a, p, half, kind).wait_send()
                second(a, p, half, kind).wait_send()
    for by in range(1, side * side):
        tell(by).wait_recv()
    total = squares[0]
    for i in range(1, side * side):
        total += squares[i]
    total = jnp.sum(jnp.sum(total, axis=1, keepdims=True), axis=0, keepdims=True)
    factor = jnp.minimum(1.0, 0.5 * lax.rsqrt(total / count + 1e-30))

    def send(a, p, ring, kind):
        direction, half, relayed = gather_kinds(ring)[kind]
        axis = 1 - p if ring == 0 else p
        along = place(axis, -direction if relayed else 0)
        other = at[1 - axis] if ring == 0 else place(1 - axis, ring - 1)
        block = whole[a].at[p, along, other] if axis == 0 else whole[a].at[p, other, along]
        if half is not None:
            block = block.at[:, columns(a, half)]
        return pltpu.make_async_remote_copy(
            src_ref=block,
            dst_ref=block,
            send_sem=gsend_sem.at[a, p, ring, kind],
            recv_sem=grecv_sem.at[a, p, ring, kind],
            device_id=device(axis, direction),
            device_id_type=MESH,
        )

    slabs = [(a, p) for a in arrays for p in PARTS]
    for a, p in slabs:
        for half in HALVES:
            cols = columns(a, half)

            def update(i, _, a=a, p=p, cols=cols):
                rows = rows_of(a, i)
                g = own[a][p, 0, at[1 - p], rows, cols].astype(F32) * factor
                w = weight[a][p, rows, cols].astype(F32)
                m = 0.9 * m_out[a][p, rows, cols] + 0.1 * g
                v = 0.95 * v_out[a][p, rows, cols] + 0.05 * g * g
                m_out[a][p, rows, cols] = m
                v_out[a][p, rows, cols] = v
                step = m * lax.rsqrt(v + 1e-8) + 0.1 * w
                whole[a][p, at[0], at[1], rows, cols] = (w - 0.02 * step).astype(jnp.bfloat16)

            lax.fori_loop(0, row_blocks(a), update, None)
        for ring in (0, 1):
            for kind in (0, 1):
                send(a, p, ring, kind).start()
    for one, then in gather_order(slabs):
        send(*one).wait_recv()
        for other in then:
            send(*other).start()
    for a, p in slabs:
        for ring in range(RINGS):
            for kind in gather_kinds(ring):
                send(a, p, ring, kind).wait_send()
    for by in range(1, side * side):
        tell(by).wait_send()


def store(*refs):
    here, there, sem = refs[:9], refs[9:18], refs[18]
    copies = [pltpu.make_async_copy(a, b, sem.at[i]) for i, (a, b) in enumerate(zip(here, there, strict=True))]
    for copy in copies:
        copy.start()
    for copy in copies:
        copy.wait()


def solution(mesh):
    devices = mesh.shape["dp"]
    side = math.isqrt(devices)

    def step(*arrays):
        terms, weights, m, v = (arrays[i : i + 3] for i in (0, 3, 6, 9))

        def blocks(x):
            return x.reshape(*x.shape[:-2], side, side, x.shape[-2] // devices, x.shape[-1])

        shapes = [one.shape for one in m]
        wholes = [blocks(w).shape for w in weights]
        count = devices * sum(math.prod(s) for s in shapes)
        out = pl.pallas_call(
            functools.partial(kernel, side, count),
            out_shape=[pltpu.VMEM(s, jnp.bfloat16) for s in wholes] + [pltpu.VMEM(s, F32) for s in shapes * 2],
            in_specs=[pl.BlockSpec(memory_space=pltpu.HBM)] * 12,
            out_specs=[pl.BlockSpec(memory_space=pltpu.VMEM)] * 9,
            scratch_shapes=[pltpu.VMEM((2, 2, side, *s[1:]), jnp.bfloat16) for s in shapes]
            + [pltpu.VMEM(s, jnp.bfloat16) for s in shapes]
            + [
                pltpu.VMEM((devices, 8, 128), F32),
                pltpu.SemaphoreType.DMA((3, 2, 5)),
                pltpu.SemaphoreType.DMA((3, 2, 2, 6)),
                pltpu.SemaphoreType.DMA((3, 2, 2, 6)),
                pltpu.SemaphoreType.DMA((3, 2, RINGS, KINDS)),
                pltpu.SemaphoreType.DMA((3, 2, RINGS, KINDS)),
                pltpu.SemaphoreType.DMA((devices - 1,)),
                pltpu.SemaphoreType.DMA((devices - 1,)),
            ],
            compiler_params=pltpu.CompilerParams(collective_id=0, has_side_effects=True, vmem_limit_bytes=20 * 2**20),
        )(*(blocks(t) for t in terms), *(blocks(w) for w in weights), *m, *v)
        out = pl.pallas_call(
            store,
            out_shape=[jax.ShapeDtypeStruct(o.shape, o.dtype) for o in out],
            in_specs=[pl.BlockSpec(memory_space=pltpu.VMEM)] * 9,
            out_specs=[pl.BlockSpec(memory_space=pltpu.HBM)] * 9,
            scratch_shapes=[pltpu.SemaphoreType.DMA((9,))],
            compiler_params=pltpu.CompilerParams(vmem_limit_bytes=20 * 2**20),
        )(*(pltpu.with_memory_space_constraint(o, pltpu.VMEM) for o in out))
        return (*(o.reshape(w.shape) for o, w in zip(out[:3], weights, strict=True)), *out[3:])

    all_of, cut = P(None, None, None), P(None, "dp", None)
    return jax.shard_map(
        step,
        mesh=mesh,
        in_specs=(P(("rep", "dp"), None, None, None),) * 3 + (all_of,) * 3 + (cut,) * 6,
        out_specs=(P("rep", None, None),) * 3 + (P("rep", "dp", None),) * 6,
        check_vma=False,
    )
```

```python
import functools
import heapq
import math

import jax
import jax.numpy as jnp
from jax import lax
from jax.experimental import pallas as pl
from jax.experimental.pallas import tpu as pltpu
from jax.sharding import PartitionSpec as P

MESH = pl.DeviceIdType.MESH
F32 = jnp.float32
LEAD_NS = 15200
PARTS = (0, 1)
HALVES = (0, 1)
RINGS = 5
KINDS = 6


def gather_kinds(ring):
    relays = {4: (1, 0, True), 5: (-1, 1, True)}
    if ring == 3:
        return {0: (1, 0, False), 1: (-1, 1, False), 2: (1, 1, False), 3: (-1, 0, False), **relays}
    return {0: (1, None, False), 1: (-1, None, False), **relays}


def gather_order(slabs):
    follow = {}
    for a, p in slabs:
        for ring in range(RINGS):
            for kind, (_, _, relayed) in gather_kinds(ring).items():
                follow[a, p, ring, kind] = [(a, p, ring, 4 + kind)] if kind < 2 else []
        for kind, k in ((0, 3), (1, 1)):
            follow[a, p, 0, kind] += [(a, p, 1 + k, 0), (a, p, 1 + k, 1)]
        follow[a, p, 0, 4] += [(a, p, 3, 0), (a, p, 3, 3)]
        follow[a, p, 0, 5] += [(a, p, 3, 1), (a, p, 3, 2)]
    free, arrivals, order, made = {}, [], [], 0

    def put(send, now):
        nonlocal made
        a, p, ring, kind = send
        direction, half, _ = gather_kinds(ring)[kind]
        way = (1 - p if ring == 0 else p, direction)
        free[way] = max(now, free.get(way, 0.0)) + (6.4 if half is None else 3.2)
        made += 1
        heapq.heappush(arrivals, (free[way] + 2.0, made, send))

    for i, (a, p) in enumerate(slabs):
        for ring in (0, 1):
            for kind in (0, 1):
                put((a, p, ring, kind), 0.4 * i)
    while arrivals:
        now, _, send = heapq.heappop(arrivals)
        order.append((send, follow[send]))
        for one in follow[send]:
            put(one, now)
    return order


def kernel(side, count, *refs):
    terms, weights, m_in, v_in, whole, m_out, v_out = (refs[3 * i : 3 * i + 3] for i in range(7))
    own, weight = refs[21:24], refs[24:27]
    squares, load_sem, send_sem, recv_sem, gsend_sem, grecv_sem, nsend_sem, nrecv_sem = refs[27:]
    arrays = range(3)
    me = lax.axis_index("dp")
    at = (me // side, me % side)

    def device(axis, by):
        moved = lax.rem(at[axis] + by + side, side)
        return {"dp": moved * side + at[1] if axis == 0 else at[0] * side + moved}

    def place(axis, by):
        return lax.rem(at[axis] + by + side, side)

    def columns(a, half):
        wide = terms[a].shape[-1] // 2
        return pl.ds(half * wide, wide)

    def row_blocks(a):
        rows = terms[a].shape[-2]
        return 3 if rows % 48 == 0 else 1

    def load(a, p, which):
        if which == 0:
            t = place(p, 0)
            source = terms[a].at[0, p, t] if p == 0 else terms[a].at[0, p, :, t]
            return pltpu.make_async_copy(source, own[a].at[p, 0], load_sem.at[a, p, 0])
        half = which - 1
        t = place(p, 1 if half == 0 else -1)
        cols = columns(a, half)
        source = terms[a].at[0, p, t, :, :, cols] if p == 0 else terms[a].at[0, p, :, t, :, cols]
        return pltpu.make_async_copy(source, own[a].at[p, 1, :, :, cols], load_sem.at[a, p, which])

    def load_state(a, which):
        if which == 0:
            return pltpu.make_async_copy(weights[a].at[:, at[0], at[1]], weight[a], load_sem.at[a, 0, 3])
        if which == 1:
            return pltpu.make_async_copy(m_in[a], m_out[a], load_sem.at[a, 1, 3])
        return pltpu.make_async_copy(v_in[a], v_out[a], load_sem.at[a, 0, 4])

    for a in arrays:
        for p in PARTS:
            for half in HALVES:
                load(a, p, 1 + half).start()

    barrier = pltpu.get_barrier_semaphore()
    for axis in (0, 1):
        for by in (1, -1):
            pl.semaphore_signal(barrier, inc=1, device_id=device(axis, by), device_id_type=MESH)
    pl.semaphore_wait(barrier, 4)
    pl.delay(lax.rem(lax.axis_index("rep"), 2) * LEAD_NS)

    def first(a, p, half, kind):
        up = 1 if half == 0 else -1
        cols = columns(a, half)
        if kind == 2:
            source, by = own[a].at[p, 1, :, :, cols], up
        else:
            by = up if kind == 0 else -up
            t = place(p, 2 if kind == 0 else by)
            source = terms[a].at[0, p, t, :, :, cols] if p == 0 else terms[a].at[0, p, :, t, :, cols]
        return pltpu.make_async_remote_copy(
            src_ref=source,
            dst_ref=whole[a].at[p, kind, :, :, cols],
            send_sem=send_sem.at[a, p, half, kind],
            recv_sem=recv_sem.at[a, p, half, kind],
            device_id=device(p, by),
            device_id_type=MESH,
        )

    def second(a, p, half, kind):
        up = 1 if half == 0 else -1
        cols = columns(a, half)
        by = -up if kind == 1 else up
        j = place(1 - p, 2 if kind == 0 else by)
        return pltpu.make_async_remote_copy(
            src_ref=own[a].at[p, 0, j, :, cols],
            dst_ref=whole[a].at[p, 3, kind, :, cols],
            send_sem=send_sem.at[a, p, half, 3 + kind],
            recv_sem=recv_sem.at[a, p, half, 3 + kind],
            device_id=device(1 - p, by),
            device_id_type=MESH,
        )

    def rows_of(a, i):
        rows = terms[a].shape[-2] // row_blocks(a)
        return pl.ds(pl.multiple_of(i * rows, rows), rows)

    def add(a, p, half, j, extra):
        cols = columns(a, half)

        def body(i, carry):
            rows = rows_of(a, i)
            total = own[a][p, 0, j, rows, cols].astype(F32)
            for k in (1, 2):
                total += whole[a][p, k, j, rows, cols].astype(F32)
            for k in extra:
                total += whole[a][p, 3, k, rows, cols].astype(F32)
            total = total.astype(jnp.bfloat16)
            own[a][p, 0, j, rows, cols] = total
            if carry is None:
                return None
            total = total.astype(F32)
            total = total * total
            total = sum(total[:, c : c + 128] for c in range(0, total.shape[1], 128))
            return carry + sum(total[r : r + 8] for r in range(0, total.shape[0], 8))

        return body

    every = [(p, half) for p in PARTS for half in HALVES]
    for a in arrays:
        for p, half in every:
            first(a, p, half, 0).start()
    for a in arrays:
        for p in PARTS:
            load(a, p, 0).start()
    for a in arrays:
        for which in range(3):
            load_state(a, which).start()
    for a in arrays:
        for p, half in every:
            first(a, p, half, 1).start()
            load(a, p, 1 + half).wait()
            first(a, p, half, 0).wait_recv()
            cols = columns(a, half)
            blocks = row_blocks(a)

            def relay(i, _, a=a, p=p, cols=cols, blocks=blocks):
                j, rows = i // blocks, rows_of(a, i % blocks)
                total = own[a][p, 1, j, rows, cols].astype(F32) + whole[a][p, 0, j, rows, cols].astype(F32)
                own[a][p, 1, j, rows, cols] = total.astype(jnp.bfloat16)

            lax.fori_loop(0, side * blocks, relay, None)
            first(a, p, half, 2).start()
    for a in arrays:
        for p in PARTS:
            load(a, p, 0).wait()
        for p, half in every:
            up = 1 if half == 0 else -1
            first(a, p, half, 1).wait_recv()
            first(a, p, half, 2).wait_recv()
            for kind in (0, 1):
                j = place(1 - p, 2 if kind == 0 else -up)
                lax.fori_loop(0, row_blocks(a), lambda i, c, f=add(a, p, half, j, ()): f(i, c), None)
                second(a, p, half, kind).start()
    for a in arrays:
        for p, half in every:
            up = 1 if half == 0 else -1
            second(a, p, half, 0).wait_recv()
            lax.fori_loop(0, row_blocks(a), lambda i, c, f=add(a, p, half, place(1 - p, up), (0,)): f(i, c), None)
            second(a, p, half, 2).start()
    total = jnp.zeros((8, 128), F32)
    for a in arrays:
        for p, half in every:
            second(a, p, half, 1).wait_recv()
            second(a, p, half, 2).wait_recv()
            total = lax.fori_loop(0, row_blocks(a), add(a, p, half, at[1 - p], (1, 2)), total)

    squares[me] = total

    def tell(by):
        return pltpu.make_async_remote_copy(
            src_ref=squares.at[me],
            dst_ref=squares.at[me],
            send_sem=nsend_sem.at[by - 1],
            recv_sem=nrecv_sem.at[by - 1],
            device_id={"dp": lax.rem(me + by, side * side)},
            device_id_type=MESH,
        )

    for by in range(1, side * side):
        tell(by).start()
    for a in arrays:
        for which in range(3):
            load_state(a, which).wait()
        for p, half in every:
            for kind in range(3):
                first(a, p, half, kind).wait_send()
                second(a, p, half, kind).wait_send()
    for by in range(1, side * side):
        tell(by).wait_recv()
    total = squares[0]
    for i in range(1, side * side):
        total += squares[i]
    total = jnp.sum(jnp.sum(total, axis=1, keepdims=True), axis=0, keepdims=True)
    factor = jnp.minimum(1.0, 0.5 * lax.rsqrt(total / count + 1e-30))

    def send(a, p, ring, kind):
        direction, half, relayed = gather_kinds(ring)[kind]
        axis = 1 - p if ring == 0 else p
        along = place(axis, -direction if relayed else 0)
        other = at[1 - axis] if ring == 0 else place(1 - axis, ring - 1)
        block = whole[a].at[p, along, other] if axis == 0 else whole[a].at[p, other, along]
        if half is not None:
            block = block.at[:, columns(a, half)]
        return pltpu.make_async_remote_copy(
            src_ref=block,
            dst_ref=block,
            send_sem=gsend_sem.at[a, p, ring, kind],
            recv_sem=grecv_sem.at[a, p, ring, kind],
            device_id=device(axis, direction),
            device_id_type=MESH,
        )

    slabs = [(a, p) for a in arrays for p in PARTS]
    for a, p in slabs:
        for half in HALVES:
            cols = columns(a, half)

            def update(i, _, a=a, p=p, cols=cols):
                rows = rows_of(a, i)
                g = own[a][p, 0, at[1 - p], rows, cols].astype(F32) * factor
                w = weight[a][p, rows, cols].astype(F32)
                m = 0.9 * m_out[a][p, rows, cols] + 0.1 * g
                v = 0.95 * v_out[a][p, rows, cols] + 0.05 * g * g
                m_out[a][p, rows, cols] = m
                v_out[a][p, rows, cols] = v
                step = m * lax.rsqrt(v + 1e-8) + 0.1 * w
                whole[a][p, at[0], at[1], rows, cols] = (w - 0.02 * step).astype(jnp.bfloat16)

            lax.fori_loop(0, row_blocks(a), update, None)
        for ring in (0, 1):
            for kind in (0, 1):
                send(a, p, ring, kind).start()
    for one, then in gather_order(slabs):
        send(*one).wait_recv()
        for other in then:
            send(*other).start()
    for a, p in slabs:
        for ring in range(RINGS):
            for kind in gather_kinds(ring):
                send(a, p, ring, kind).wait_send()
    for by in range(1, side * side):
        tell(by).wait_send()


def store(*refs):
    here, there, sem = refs[:9], refs[9:18], refs[18]
    copies = [pltpu.make_async_copy(a, b, sem.at[i]) for i, (a, b) in enumerate(zip(here, there, strict=True))]
    for copy in copies:
        copy.start()
    for copy in copies:
        copy.wait()


def solution(mesh):
    devices = mesh.shape["dp"]
    side = math.isqrt(devices)

    def step(*arrays):
        terms, weights, m, v = (arrays[i : i + 3] for i in (0, 3, 6, 9))

        def blocks(x):
            return x.reshape(*x.shape[:-2], side, side, x.shape[-2] // devices, x.shape[-1])

        shapes = [one.shape for one in m]
        wholes = [blocks(w).shape for w in weights]
        count = devices * sum(math.prod(s) for s in shapes)
        out = pl.pallas_call(
            functools.partial(kernel, side, count),
            out_shape=[pltpu.VMEM(s, jnp.bfloat16) for s in wholes] + [pltpu.VMEM(s, F32) for s in shapes * 2],
            in_specs=[pl.BlockSpec(memory_space=pltpu.HBM)] * 12,
            out_specs=[pl.BlockSpec(memory_space=pltpu.VMEM)] * 9,
            scratch_shapes=[pltpu.VMEM((2, 2, side, *s[1:]), jnp.bfloat16) for s in shapes]
            + [pltpu.VMEM(s, jnp.bfloat16) for s in shapes]
            + [
                pltpu.VMEM((devices, 8, 128), F32),
                pltpu.SemaphoreType.DMA((3, 2, 5)),
                pltpu.SemaphoreType.DMA((3, 2, 2, 6)),
                pltpu.SemaphoreType.DMA((3, 2, 2, 6)),
                pltpu.SemaphoreType.DMA((3, 2, RINGS, KINDS)),
                pltpu.SemaphoreType.DMA((3, 2, RINGS, KINDS)),
                pltpu.SemaphoreType.DMA((devices - 1,)),
                pltpu.SemaphoreType.DMA((devices - 1,)),
            ],
            compiler_params=pltpu.CompilerParams(collective_id=0, has_side_effects=True, vmem_limit_bytes=20 * 2**20),
        )(*(blocks(t) for t in terms), *(blocks(w) for w in weights), *m, *v)
        out = pl.pallas_call(
            store,
            out_shape=[jax.ShapeDtypeStruct(o.shape, o.dtype) for o in out],
            in_specs=[pl.BlockSpec(memory_space=pltpu.VMEM)] * 9,
            out_specs=[pl.BlockSpec(memory_space=pltpu.HBM)] * 9,
            scratch_shapes=[pltpu.SemaphoreType.DMA((9,))],
            compiler_params=pltpu.CompilerParams(vmem_limit_bytes=20 * 2**20),
        )(*(pltpu.with_memory_space_constraint(o, pltpu.VMEM) for o in out))
        return (*(o.reshape(w.shape) for o, w in zip(out[:3], weights, strict=True)), *out[3:])

    all_of, cut = P(None, None, None), P(None, "dp", None)
    return jax.shard_map(
        step,
        mesh=mesh,
        in_specs=(P(("rep", "dp"), None, None, None),) * 3 + (all_of,) * 3 + (cut,) * 6,
        out_specs=(P("rep", None, None),) * 3 + (P("rep", "dp", None),) * 6,
        check_vma=False,
    )
```

```python
import functools
import heapq
import math

import jax
import jax.numpy as jnp
from jax import lax
from jax.experimental import pallas as pl
from jax.experimental.pallas import tpu as pltpu
from jax.sharding import PartitionSpec as P

MESH = pl.DeviceIdType.MESH
F32 = jnp.float32
LEAD_NS = 25000
VMEM = 27 * 2**20
PARTS = (0, 1)
HALVES = (0, 1)
RINGS = 5
KINDS = 6


def gather_kinds(ring):
    relays = {4: (1, 0, True), 5: (-1, 1, True)}
    if ring == 3:
        return {0: (1, 0, False), 1: (-1, 1, False), 2: (1, 1, False), 3: (-1, 0, False), **relays}
    return {0: (1, None, False), 1: (-1, None, False), **relays}


def gather_order(slabs):
    follow = {}
    for a, p in slabs:
        for ring in range(RINGS):
            for kind, (_, _, relayed) in gather_kinds(ring).items():
                follow[a, p, ring, kind] = [(a, p, ring, 4 + kind)] if kind < 2 else []
        for kind, k in ((0, 3), (1, 1)):
            follow[a, p, 0, kind] += [(a, p, 1 + k, 0), (a, p, 1 + k, 1)]
        follow[a, p, 0, 4] += [(a, p, 3, 0), (a, p, 3, 3)]
        follow[a, p, 0, 5] += [(a, p, 3, 1), (a, p, 3, 2)]
    free, arrivals, order, made = {}, [], [], 0

    def put(send, now):
        nonlocal made
        a, p, ring, kind = send
        direction, half, _ = gather_kinds(ring)[kind]
        way = (1 - p if ring == 0 else p, direction)
        free[way] = max(now, free.get(way, 0.0)) + (6.4 if half is None else 3.2)
        made += 1
        heapq.heappush(arrivals, (free[way] + 2.0, made, send))

    for i, (a, p) in enumerate(slabs):
        for ring in (0, 1):
            for kind in (0, 1):
                put((a, p, ring, kind), 0.4 * i)
    while arrivals:
        now, _, send = heapq.heappop(arrivals)
        order.append((send, follow[send]))
        for one in follow[send]:
            put(one, now)
    return order


def moved(side, at, axis, by):
    return lax.rem(at[axis] + by + side, side)


def device(side, at, axis, by):
    to = moved(side, at, axis, by)
    return {"dp": to * side + at[1] if axis == 0 else at[0] * side + to}


def columns(wide, half):
    return pl.ds(half * (wide // 2), wide // 2)


def meet(side, at):
    barrier = pltpu.get_barrier_semaphore()
    for axis in (0, 1):
        for by in (1, -1):
            pl.semaphore_signal(barrier, inc=1, device_id=device(side, at, axis, by), device_id_type=MESH)
    pl.semaphore_wait(barrier, 4)


def gather_copy(side, at, whole, sems, part, ring, kind, own=None):
    direction, half, relayed = gather_kinds(ring)[kind]
    axis = 1 - part if ring == 0 else part
    along = moved(side, at, axis, -direction if relayed else 0)
    other = at[1 - axis] if ring == 0 else moved(side, at, 1 - axis, ring - 1)
    block = whole.at[part, along, other] if axis == 0 else whole.at[part, other, along]
    if half is not None:
        block = block.at[:, columns(whole.shape[-1], half)]
    return pltpu.make_async_remote_copy(
        src_ref=own.at[part] if own is not None and ring < 2 and not relayed else block,
        dst_ref=block,
        send_sem=sems[0].at[part, ring, kind],
        recv_sem=sems[1].at[part, ring, kind],
        device_id=device(side, at, axis, direction),
        device_id_type=MESH,
    )


def sum_and_step(side, count, *refs):
    terms, weights, m_in, v_in = (refs[3 * i : 3 * i + 3] for i in range(4))
    fresh = refs[14]
    m_out, v_out, own, weight = (refs[15 + 3 * i : 18 + 3 * i] for i in range(4))
    slots = (*refs[12:14], refs[27])
    squares, load_sem, send_sem, recv_sem, gsend_sem, grecv_sem, nsend_sem, nrecv_sem = refs[28:]
    arrays = range(3)
    me = lax.axis_index("dp")
    at = (me // side, me % side)

    def place(axis, by):
        return moved(side, at, axis, by)

    def half_of(a, half):
        return columns(terms[a].shape[-1], half)

    def row_blocks(a):
        rows = terms[a].shape[-2]
        return 3 if rows % 48 == 0 else 1

    def load(a, p, which):
        if which == 0:
            t = place(p, 0)
            source = terms[a].at[0, p, t] if p == 0 else terms[a].at[0, p, :, t]
            return pltpu.make_async_copy(source, own[a].at[p, 0], load_sem.at[a, p, 0])
        half = which - 1
        t = place(p, 1 if half == 0 else -1)
        cols = half_of(a, half)
        source = terms[a].at[0, p, t, :, :, cols] if p == 0 else terms[a].at[0, p, :, t, :, cols]
        return pltpu.make_async_copy(source, own[a].at[p, 1, :, :, cols], load_sem.at[a, p, which])

    def load_state(a, which):
        if which == 0:
            return pltpu.make_async_copy(weights[a].at[:, at[0], at[1]], weight[a], load_sem.at[a, 0, 3])
        if which == 1:
            return pltpu.make_async_copy(m_in[a], m_out[a], load_sem.at[a, 1, 3])
        return pltpu.make_async_copy(v_in[a], v_out[a], load_sem.at[a, 0, 4])

    for a in arrays:
        for p in PARTS:
            for half in HALVES:
                load(a, p, 1 + half).start()

    meet(side, at)
    pl.delay(lax.rem(lax.axis_index("rep"), 2) * LEAD_NS)

    def first(a, p, half, kind):
        up = 1 if half == 0 else -1
        cols = half_of(a, half)
        if kind == 2:
            source, by = own[a].at[p, 1, :, :, cols], up
        else:
            by = up if kind == 0 else -up
            t = place(p, 2 if kind == 0 else by)
            source = terms[a].at[0, p, t, :, :, cols] if p == 0 else terms[a].at[0, p, :, t, :, cols]
        return pltpu.make_async_remote_copy(
            src_ref=source,
            dst_ref=slots[a].at[p, kind, :, :, cols],
            send_sem=send_sem.at[a, p, half, kind],
            recv_sem=recv_sem.at[a, p, half, kind],
            device_id=device(side, at, p, by),
            device_id_type=MESH,
        )

    def second(a, p, half, kind):
        up = 1 if half == 0 else -1
        cols = half_of(a, half)
        by = -up if kind == 1 else up
        j = place(1 - p, 2 if kind == 0 else by)
        return pltpu.make_async_remote_copy(
            src_ref=own[a].at[p, 0, j, :, cols],
            dst_ref=slots[a].at[p, 3, kind, :, cols],
            send_sem=send_sem.at[a, p, half, 3 + kind],
            recv_sem=recv_sem.at[a, p, half, 3 + kind],
            device_id=device(side, at, 1 - p, by),
            device_id_type=MESH,
        )

    def rows_of(a, i):
        rows = terms[a].shape[-2] // row_blocks(a)
        return pl.ds(pl.multiple_of(i * rows, rows), rows)

    def add(a, p, half, j, extra):
        cols = half_of(a, half)

        def body(i, carry):
            rows = rows_of(a, i)
            total = own[a][p, 0, j, rows, cols].astype(F32)
            for k in (1, 2):
                total += slots[a][p, k, j, rows, cols].astype(F32)
            for k in extra:
                total += slots[a][p, 3, k, rows, cols].astype(F32)
            total = total.astype(jnp.bfloat16)
            own[a][p, 0, j, rows, cols] = total
            if carry is None:
                return None
            total = total.astype(F32)
            total = total * total
            total = sum(total[:, c : c + 128] for c in range(0, total.shape[1], 128))
            return carry + sum(total[r : r + 8] for r in range(0, total.shape[0], 8))

        return body

    every = [(p, half) for p in PARTS for half in HALVES]
    for a in arrays:
        for p, half in every:
            first(a, p, half, 0).start()
    for a in arrays:
        for p in PARTS:
            load(a, p, 0).start()
    for a in arrays:
        for which in range(3):
            load_state(a, which).start()
    for a in arrays:
        for p, half in every:
            first(a, p, half, 1).start()
            load(a, p, 1 + half).wait()
            first(a, p, half, 0).wait_recv()
            cols = half_of(a, half)
            blocks = row_blocks(a)

            def relay(i, _, a=a, p=p, cols=cols, blocks=blocks):
                j, rows = i // blocks, rows_of(a, i % blocks)
                total = own[a][p, 1, j, rows, cols].astype(F32) + slots[a][p, 0, j, rows, cols].astype(F32)
                own[a][p, 1, j, rows, cols] = total.astype(jnp.bfloat16)

            lax.fori_loop(0, side * blocks, relay, None)
            first(a, p, half, 2).start()
    for a in arrays:
        for p in PARTS:
            load(a, p, 0).wait()
        for p, half in every:
            up = 1 if half == 0 else -1
            first(a, p, half, 1).wait_recv()
            first(a, p, half, 2).wait_recv()
            for kind in (0, 1):
                j = place(1 - p, 2 if kind == 0 else -up)
                lax.fori_loop(0, row_blocks(a), lambda i, c, f=add(a, p, half, j, ()): f(i, c), None)
                second(a, p, half, kind).start()
    for a in arrays:
        for p, half in every:
            up = 1 if half == 0 else -1
            second(a, p, half, 0).wait_recv()
            lax.fori_loop(0, row_blocks(a), lambda i, c, f=add(a, p, half, place(1 - p, up), (0,)): f(i, c), None)
            second(a, p, half, 2).start()
    total = jnp.zeros((8, 128), F32)
    for a in arrays:
        for p, half in every:
            second(a, p, half, 1).wait_recv()
            second(a, p, half, 2).wait_recv()
            total = lax.fori_loop(0, row_blocks(a), add(a, p, half, at[1 - p], (1, 2)), total)

    squares[me] = total

    def tell(by):
        return pltpu.make_async_remote_copy(
            src_ref=squares.at[me],
            dst_ref=squares.at[me],
            send_sem=nsend_sem.at[by - 1],
            recv_sem=nrecv_sem.at[by - 1],
            device_id={"dp": lax.rem(me + by, side * side)},
            device_id_type=MESH,
        )

    for by in range(1, side * side):
        tell(by).start()
    for a in arrays:
        for which in range(3):
            load_state(a, which).wait()
        for p, half in every:
            for kind in range(3):
                first(a, p, half, kind).wait_send()
                second(a, p, half, kind).wait_send()
    for by in range(1, side * side):
        tell(by).wait_recv()
    total = squares[0]
    for i in range(1, side * side):
        total += squares[i]
    total = jnp.sum(jnp.sum(total, axis=1, keepdims=True), axis=0, keepdims=True)
    factor = jnp.minimum(1.0, 0.5 * lax.rsqrt(total / count + 1e-30))

    def send(a, *which):
        return gather_copy(side, at, slots[a], (gsend_sem.at[a], grecv_sem.at[a]), *which)

    for a in arrays:
        for p in PARTS:
            for half in HALVES:
                cols = half_of(a, half)

                def update(i, _, a=a, p=p, cols=cols):
                    rows = rows_of(a, i)
                    g = own[a][p, 0, at[1 - p], rows, cols].astype(F32) * factor
                    w = weight[a][p, rows, cols].astype(F32)
                    m = 0.9 * m_out[a][p, rows, cols] + 0.1 * g
                    v = 0.95 * v_out[a][p, rows, cols] + 0.05 * g * g
                    m_out[a][p, rows, cols] = m
                    v_out[a][p, rows, cols] = v
                    step = m * lax.rsqrt(v + 1e-8) + 0.1 * w
                    w = (w - 0.02 * step).astype(jnp.bfloat16)
                    if a == 2:
                        fresh[p, rows, cols] = w
                    else:
                        slots[a][p, at[0], at[1], rows, cols] = w

                lax.fori_loop(0, row_blocks(a), update, None)
            if a < 2:
                for ring in (0, 1):
                    for kind in (0, 1):
                        send(a, p, ring, kind).start()
    slabs = [(a, p) for a in (0, 1) for p in PARTS]
    for one, then in gather_order(slabs):
        send(*one).wait_recv()
        for other in then:
            send(*other).start()
    for a, p in slabs:
        for ring in range(RINGS):
            for kind in gather_kinds(ring):
                send(a, p, ring, kind).wait_send()
    for by in range(1, side * side):
        tell(by).wait_send()


def gather_last(side, fresh, whole, send_sem, recv_sem, copy_sem):
    me = lax.axis_index("dp")
    at = (me // side, me % side)
    keep = [pltpu.make_async_copy(fresh.at[p], whole.at[p, at[0], at[1]], copy_sem.at[p]) for p in PARTS]
    for p in PARTS:
        keep[p].start()
    meet(side, at)

    def send(_, *which):
        return gather_copy(side, at, whole, (send_sem, recv_sem), *which, own=fresh)

    slabs = [(0, p) for p in PARTS]
    for a, p in slabs:
        for ring in (0, 1):
            for kind in (0, 1):
                send(a, p, ring, kind).start()
    for one, then in gather_order(slabs):
        send(*one).wait_recv()
        for other in then:
            send(*other).start()
    for p in PARTS:
        keep[p].wait()
        for ring in range(RINGS):
            for kind in gather_kinds(ring):
                send(0, p, ring, kind).wait_send()


def store(arrays, vmem):
    def body(*refs):
        here, there, sem = refs[: len(arrays)], refs[len(arrays) : -1], refs[-1]
        copies = [pltpu.make_async_copy(a, b, sem.at[i]) for i, (a, b) in enumerate(zip(here, there, strict=True))]
        for copy in copies:
            copy.start()
        for copy in copies:
            copy.wait()

    return pl.pallas_call(
        body,
        out_shape=[pltpu.HBM(x.shape, x.dtype) for x in arrays],
        in_specs=[pl.BlockSpec(memory_space=pltpu.VMEM)] * len(arrays),
        out_specs=[pl.BlockSpec(memory_space=pltpu.HBM)] * len(arrays),
        scratch_shapes=[pltpu.SemaphoreType.DMA((len(arrays),))],
        compiler_params=pltpu.CompilerParams(vmem_limit_bytes=vmem),
    )(*(pltpu.with_memory_space_constraint(x, pltpu.VMEM) for x in arrays))


def solution(mesh):
    devices = mesh.shape["dp"]
    side = math.isqrt(devices)

    def step(*arrays):
        terms, weights, m, v = (arrays[i : i + 3] for i in (0, 3, 6, 9))

        def blocks(x):
            return x.reshape(*x.shape[:-2], side, side, x.shape[-2] // devices, x.shape[-1])

        def here(shape, dtype):
            return pltpu.VMEM(shape, dtype)

        shapes = [one.shape for one in m]
        wholes = [blocks(w).shape for w in weights]
        count = devices * sum(math.prod(s) for s in shapes)
        gather_sems = [pltpu.SemaphoreType.DMA((2, RINGS, KINDS))] * 2
        new = pl.pallas_call(
            functools.partial(sum_and_step, side, count),
            out_shape=[here(s, jnp.bfloat16) for s in (*wholes[:2], shapes[2])] + [here(s, F32) for s in shapes * 2],
            in_specs=[pl.BlockSpec(memory_space=pltpu.HBM)] * 12,
            out_specs=[pl.BlockSpec(memory_space=pltpu.VMEM)] * 9,
            scratch_shapes=[pltpu.VMEM((2, 2, side, *s[1:]), jnp.bfloat16) for s in shapes]
            + [pltpu.VMEM(s, jnp.bfloat16) for s in (*shapes, wholes[2])]
            + [
                pltpu.VMEM((devices, 8, 128), F32),
                pltpu.SemaphoreType.DMA((3, 2, 5)),
                pltpu.SemaphoreType.DMA((3, 2, 2, 6)),
                pltpu.SemaphoreType.DMA((3, 2, 2, 6)),
                pltpu.SemaphoreType.DMA((2, 2, RINGS, KINDS)),
                pltpu.SemaphoreType.DMA((2, 2, RINGS, KINDS)),
                pltpu.SemaphoreType.DMA((devices - 1,)),
                pltpu.SemaphoreType.DMA((devices - 1,)),
            ],
            compiler_params=pltpu.CompilerParams(collective_id=0, has_side_effects=True, vmem_limit_bytes=VMEM),
        )(*(pltpu.with_memory_space_constraint(x, pltpu.HBM) for x in (*map(blocks, terms), *map(blocks, weights), *m, *v)))
        new = store(new, VMEM)
        last = pl.pallas_call(
            functools.partial(gather_last, side),
            out_shape=here(wholes[2], jnp.bfloat16),
            in_specs=[pl.BlockSpec(memory_space=pltpu.HBM)],
            out_specs=pl.BlockSpec(memory_space=pltpu.VMEM),
            scratch_shapes=[*gather_sems, pltpu.SemaphoreType.DMA((2,))],
            compiler_params=pltpu.CompilerParams(collective_id=1, has_side_effects=True, vmem_limit_bytes=VMEM),
        )(pltpu.with_memory_space_constraint(new[2], pltpu.HBM))
        (last,) = store([last], VMEM)
        return (*(o.reshape(w.shape) for o, w in zip((*new[:2], last), weights, strict=True)), *new[3:])

    all_of, cut = P(None, None, None), P(None, "dp", None)
    return jax.shard_map(
        step,
        mesh=mesh,
        in_specs=(P(("rep", "dp"), None, None, None),) * 3 + (all_of,) * 3 + (cut,) * 6,
        out_specs=(P("rep", None, None),) * 3 + (P("rep", "dp", None),) * 6,
        check_vma=False,
    )
```

```python
import functools
import heapq
import math

import jax
import jax.numpy as jnp
from jax import lax
from jax.experimental import pallas as pl
from jax.experimental.pallas import tpu as pltpu
from jax.sharding import PartitionSpec as P

MESH = pl.DeviceIdType.MESH
F32 = jnp.float32
LEAD_NS = 23500
VMEM = 27 * 2**20
PARTS = (0, 1)
HALVES = (0, 1)
RINGS = 5
KINDS = 6


def gather_kinds(ring, fine):
    relays = {4: (1, 0, True), 5: (-1, 1, True)}
    if fine and ring == 3:
        return {0: (1, 0, False), 1: (-1, 1, False), 2: (1, 1, False), 3: (-1, 0, False), **relays}
    return {0: (1, None, False), 1: (-1, None, False), **relays}


def gather_order(slabs, fine):
    follow, waits = {}, {}
    for a, p in slabs:
        for ring in range(RINGS if fine else 2):
            for kind, (_, _, relayed) in gather_kinds(ring, fine).items():
                follow[a, p, ring, kind] = [(a, p, ring, 4 + kind)] if kind < 2 else []
        if fine:
            for kind, k in ((0, 3), (1, 1)):
                follow[a, p, 0, kind] += [(a, p, 1 + k, 0), (a, p, 1 + k, 1)]
            follow[a, p, 0, 4] += [(a, p, 3, 0), (a, p, 3, 3)]
            follow[a, p, 0, 5] += [(a, p, 3, 1), (a, p, 3, 2)]
        else:
            waits[a, p] = 4
    free, arrivals, order, made = {}, [], [], 0

    def put(send, now):
        nonlocal made
        a, p, ring, kind = send
        direction, half, _ = gather_kinds(ring, fine)[kind]
        way = (1 - p if ring == 0 else p, direction)
        time = (6.4 if half is None else 3.2) * (1 if fine or ring == 0 else 4)
        free[way] = max(now, free.get(way, 0.0)) + time
        made += 1
        heapq.heappush(arrivals, (free[way] + 2.0, made, send))

    for i, (a, p) in enumerate(slabs):
        for ring in (0, 1) if fine else (0,):
            for kind in (0, 1):
                put((a, p, ring, kind), 0.4 * i)
    while arrivals:
        now, _, send = heapq.heappop(arrivals)
        then = list(follow[send])
        if send[2] == 0 and not fine:
            waits[send[:2]] -= 1
            if waits[send[:2]] == 0:
                then += [(*send[:2], 1, 0), (*send[:2], 1, 1)]
        order.append((send, then))
        for one in then:
            put(one, now)
    return order


def moved(side, at, axis, by):
    return lax.rem(at[axis] + by + side, side)


def device(side, at, axis, by):
    to = moved(side, at, axis, by)
    return {"dp": to * side + at[1] if axis == 0 else at[0] * side + to}


def columns(wide, half):
    return pl.ds(half * (wide // 2), wide // 2)


def meet(side, at):
    barrier = pltpu.get_barrier_semaphore()
    for axis in (0, 1):
        for by in (1, -1):
            pl.semaphore_signal(barrier, inc=1, device_id=device(side, at, axis, by), device_id_type=MESH)
    pl.semaphore_wait(barrier, 4)


def gather_copy(side, at, whole, sems, fine, part, ring, kind, own=None):
    direction, half, relayed = gather_kinds(ring, fine)[kind]
    axis = 1 - part if ring == 0 else part
    along = moved(side, at, axis, -direction if relayed else 0)
    if ring == 1 and not fine:
        block = whole.at[part, along] if axis == 0 else whole.at[part, :, along]
        if half is not None:
            block = block.at[:, :, columns(whole.shape[-1], half)]
    else:
        other = at[1 - axis] if ring == 0 else moved(side, at, 1 - axis, ring - 1)
        block = whole.at[part, along, other] if axis == 0 else whole.at[part, other, along]
        if half is not None:
            block = block.at[:, columns(whole.shape[-1], half)]
    return pltpu.make_async_remote_copy(
        src_ref=own.at[part] if own is not None and ring < 2 and not relayed else block,
        dst_ref=block,
        send_sem=sems[0].at[part, ring, kind],
        recv_sem=sems[1].at[part, ring, kind],
        device_id=device(side, at, axis, direction),
        device_id_type=MESH,
    )


def sum_and_step(side, count, *refs):
    terms, weights, m_in, v_in = (refs[3 * i : 3 * i + 3] for i in range(4))
    fresh = refs[14]
    m_out, v_out, own, weight = (refs[15 + 3 * i : 18 + 3 * i] for i in range(4))
    slots = (*refs[12:14], refs[27])
    squares, load_sem, send_sem, recv_sem, gsend_sem, grecv_sem, nsend_sem, nrecv_sem = refs[28:]
    arrays = range(3)
    me = lax.axis_index("dp")
    at = (me // side, me % side)

    def place(axis, by):
        return moved(side, at, axis, by)

    def half_of(a, half):
        return columns(terms[a].shape[-1], half)

    def row_blocks(a):
        rows = terms[a].shape[-2]
        return 3 if rows % 48 == 0 else 1

    def load(a, p, which):
        if which == 0:
            t = place(p, 0)
            source = terms[a].at[0, p, t] if p == 0 else terms[a].at[0, p, :, t]
            return pltpu.make_async_copy(source, own[a].at[p, 0], load_sem.at[a, p, 0])
        half = which - 1
        t = place(p, 1 if half == 0 else -1)
        cols = half_of(a, half)
        source = terms[a].at[0, p, t, :, :, cols] if p == 0 else terms[a].at[0, p, :, t, :, cols]
        return pltpu.make_async_copy(source, own[a].at[p, 1, :, :, cols], load_sem.at[a, p, which])

    def load_state(a, which):
        if which == 0:
            return pltpu.make_async_copy(weights[a].at[:, at[0], at[1]], weight[a], load_sem.at[a, 0, 3])
        if which == 1:
            return pltpu.make_async_copy(m_in[a], m_out[a], load_sem.at[a, 1, 3])
        return pltpu.make_async_copy(v_in[a], v_out[a], load_sem.at[a, 0, 4])

    meet(side, at)
    pl.delay(lax.rem(lax.axis_index("rep"), 2) * LEAD_NS)

    def first(a, p, half, kind):
        up = 1 if half == 0 else -1
        cols = half_of(a, half)
        if kind == 2:
            source, by = own[a].at[p, 1, :, :, cols], up
        else:
            by = up if kind == 0 else -up
            t = place(p, 2 if kind == 0 else by)
            source = terms[a].at[0, p, t, :, :, cols] if p == 0 else terms[a].at[0, p, :, t, :, cols]
        return pltpu.make_async_remote_copy(
            src_ref=source,
            dst_ref=slots[a].at[p, kind, :, :, cols],
            send_sem=send_sem.at[a, p, half, kind],
            recv_sem=recv_sem.at[a, p, half, kind],
            device_id=device(side, at, p, by),
            device_id_type=MESH,
        )

    def second(a, p, half, kind):
        up = 1 if half == 0 else -1
        cols = half_of(a, half)
        by = -up if kind == 1 else up
        j = place(1 - p, 2 if kind == 0 else by)
        return pltpu.make_async_remote_copy(
            src_ref=own[a].at[p, 0, j, :, cols],
            dst_ref=slots[a].at[p, 3, kind, :, cols],
            send_sem=send_sem.at[a, p, half, 3 + kind],
            recv_sem=recv_sem.at[a, p, half, 3 + kind],
            device_id=device(side, at, 1 - p, by),
            device_id_type=MESH,
        )

    def rows_of(a, i):
        rows = terms[a].shape[-2] // row_blocks(a)
        return pl.ds(pl.multiple_of(i * rows, rows), rows)

    def add(a, p, half, j, extra):
        cols = half_of(a, half)

        def body(i, carry):
            rows = rows_of(a, i)
            total = own[a][p, 0, j, rows, cols].astype(F32)
            for k in (1, 2):
                total += slots[a][p, k, j, rows, cols].astype(F32)
            for k in extra:
                total += slots[a][p, 3, k, rows, cols].astype(F32)
            total = total.astype(jnp.bfloat16)
            own[a][p, 0, j, rows, cols] = total
            if carry is None:
                return None
            total = total.astype(F32)
            total = total * total
            total = sum(total[:, c : c + 128] for c in range(0, total.shape[1], 128))
            return carry + sum(total[r : r + 8] for r in range(0, total.shape[0], 8))

        return body

    every = [(p, half) for p in PARTS for half in HALVES]
    for a in arrays:
        for p, half in every:
            first(a, p, half, 0).start()
    for a in arrays:
        for p, half in every:
            load(a, p, 1 + half).start()
    for a in arrays:
        for p in PARTS:
            load(a, p, 0).start()
    for a in arrays:
        for which in range(3):
            load_state(a, which).start()
    for a in arrays:
        for p, half in every:
            first(a, p, half, 1).start()
            load(a, p, 1 + half).wait()
            first(a, p, half, 0).wait_recv()
            cols = half_of(a, half)
            blocks = row_blocks(a)

            def relay(i, _, a=a, p=p, cols=cols, blocks=blocks):
                j, rows = i // blocks, rows_of(a, i % blocks)
                total = own[a][p, 1, j, rows, cols].astype(F32) + slots[a][p, 0, j, rows, cols].astype(F32)
                own[a][p, 1, j, rows, cols] = total.astype(jnp.bfloat16)

            lax.fori_loop(0, side * blocks, relay, None)
            first(a, p, half, 2).start()
    for a in arrays:
        for p in PARTS:
            load(a, p, 0).wait()
        for p, half in every:
            up = 1 if half == 0 else -1
            first(a, p, half, 1).wait_recv()
            first(a, p, half, 2).wait_recv()
            for kind in (0, 1):
                j = place(1 - p, 2 if kind == 0 else -up)
                lax.fori_loop(0, row_blocks(a), lambda i, c, f=add(a, p, half, j, ()): f(i, c), None)
                second(a, p, half, kind).start()
    for a in arrays:
        for p, half in every:
            up = 1 if half == 0 else -1
            second(a, p, half, 0).wait_recv()
            lax.fori_loop(0, row_blocks(a), lambda i, c, f=add(a, p, half, place(1 - p, up), (0,)): f(i, c), None)
            second(a, p, half, 2).start()
    total = jnp.zeros((8, 128), F32)
    for a in arrays:
        for p, half in every:
            second(a, p, half, 1).wait_recv()
            second(a, p, half, 2).wait_recv()
            total = lax.fori_loop(0, row_blocks(a), add(a, p, half, at[1 - p], (1, 2)), total)

    squares[me] = jnp.sum(total, axis=0, keepdims=True)

    def tell(by):
        return pltpu.make_async_remote_copy(
            src_ref=squares.at[me],
            dst_ref=squares.at[me],
            send_sem=nsend_sem.at[by - 1],
            recv_sem=nrecv_sem.at[by - 1],
            device_id={"dp": lax.rem(me + by, side * side)},
            device_id_type=MESH,
        )

    for by in range(1, side * side):
        tell(by).start()
    for a in arrays:
        for which in range(3):
            load_state(a, which).wait()
        for p, half in every:
            for kind in range(3):
                first(a, p, half, kind).wait_send()
                second(a, p, half, kind).wait_send()
    for by in range(1, side * side):
        tell(by).wait_recv()
    total = squares[0]
    for i in range(1, side * side):
        total += squares[i]
    total = jnp.sum(total, axis=1, keepdims=True)
    factor = jnp.minimum(1.0, 0.5 * lax.rsqrt(total / count + 1e-30))

    def send(a, *which):
        return gather_copy(side, at, slots[a], (gsend_sem.at[a], grecv_sem.at[a]), False, *which)

    for a in arrays:
        for p in PARTS:
            for half in HALVES:
                cols = half_of(a, half)

                def update(i, _, a=a, p=p, cols=cols):
                    rows = rows_of(a, i)
                    g = own[a][p, 0, at[1 - p], rows, cols].astype(F32) * factor
                    w = weight[a][p, rows, cols].astype(F32)
                    m = 0.9 * m_out[a][p, rows, cols] + 0.1 * g
                    v = 0.95 * v_out[a][p, rows, cols] + 0.05 * g * g
                    m_out[a][p, rows, cols] = m
                    v_out[a][p, rows, cols] = v
                    step = m * lax.rsqrt(v + 1e-8) + 0.1 * w
                    w = (w - 0.02 * step).astype(jnp.bfloat16)
                    if a == 2:
                        fresh[p, rows, cols] = w
                    else:
                        slots[a][p, at[0], at[1], rows, cols] = w

                lax.fori_loop(0, row_blocks(a), update, None)
            if a < 2:
                for kind in (0, 1):
                    send(a, p, 0, kind).start()
    slabs = [(a, p) for a in (0, 1) for p in PARTS]
    for one, then in gather_order(slabs, False):
        send(*one).wait_recv()
        for other in then:
            send(*other).start()
    for a, p in slabs:
        for ring in (0, 1):
            for kind in gather_kinds(ring, False):
                send(a, p, ring, kind).wait_send()
    for by in range(1, side * side):
        tell(by).wait_send()


def gather_last(side, fresh, whole, send_sem, recv_sem, copy_sem):
    me = lax.axis_index("dp")
    at = (me // side, me % side)
    keep = [pltpu.make_async_copy(fresh.at[p], whole.at[p, at[0], at[1]], copy_sem.at[p]) for p in PARTS]
    for p in PARTS:
        keep[p].start()
    meet(side, at)

    def send(_, *which):
        return gather_copy(side, at, whole, (send_sem, recv_sem), True, *which, own=fresh)

    slabs = [(0, p) for p in PARTS]
    for a, p in slabs:
        for ring in (0, 1):
            for kind in (0, 1):
                send(a, p, ring, kind).start()
    for one, then in gather_order(slabs, True):
        send(*one).wait_recv()
        for other in then:
            send(*other).start()
    for p in PARTS:
        keep[p].wait()
        for ring in range(RINGS):
            for kind in gather_kinds(ring, True):
                send(0, p, ring, kind).wait_send()


def store(arrays, vmem):
    def body(*refs):
        here, there, sem = refs[: len(arrays)], refs[len(arrays) : -1], refs[-1]
        copies = [pltpu.make_async_copy(a, b, sem.at[i]) for i, (a, b) in enumerate(zip(here, there, strict=True))]
        for copy in copies:
            copy.start()
        for copy in copies:
            copy.wait()

    return pl.pallas_call(
        body,
        out_shape=[pltpu.HBM(x.shape, x.dtype) for x in arrays],
        in_specs=[pl.BlockSpec(memory_space=pltpu.VMEM)] * len(arrays),
        out_specs=[pl.BlockSpec(memory_space=pltpu.HBM)] * len(arrays),
        scratch_shapes=[pltpu.SemaphoreType.DMA((len(arrays),))],
        compiler_params=pltpu.CompilerParams(vmem_limit_bytes=vmem),
    )(*(pltpu.with_memory_space_constraint(x, pltpu.VMEM) for x in arrays))


def solution(mesh):
    devices = mesh.shape["dp"]
    side = math.isqrt(devices)

    def step(*arrays):
        terms, weights, m, v = (arrays[i : i + 3] for i in (0, 3, 6, 9))

        def blocks(x):
            return x.reshape(*x.shape[:-2], side, side, x.shape[-2] // devices, x.shape[-1])

        def here(shape, dtype):
            return pltpu.VMEM(shape, dtype)

        shapes = [one.shape for one in m]
        wholes = [blocks(w).shape for w in weights]
        count = devices * sum(math.prod(s) for s in shapes)
        gather_sems = [pltpu.SemaphoreType.DMA((2, RINGS, KINDS))] * 2
        new = pl.pallas_call(
            functools.partial(sum_and_step, side, count),
            out_shape=[here(s, jnp.bfloat16) for s in (*wholes[:2], shapes[2])] + [here(s, F32) for s in shapes * 2],
            in_specs=[pl.BlockSpec(memory_space=pltpu.HBM)] * 12,
            out_specs=[pl.BlockSpec(memory_space=pltpu.VMEM)] * 9,
            scratch_shapes=[pltpu.VMEM((2, 2, side, *s[1:]), jnp.bfloat16) for s in shapes]
            + [pltpu.VMEM(s, jnp.bfloat16) for s in (*shapes, wholes[2])]
            + [
                pltpu.VMEM((devices, 1, 128), F32),
                pltpu.SemaphoreType.DMA((3, 2, 5)),
                pltpu.SemaphoreType.DMA((3, 2, 2, 6)),
                pltpu.SemaphoreType.DMA((3, 2, 2, 6)),
                pltpu.SemaphoreType.DMA((2, 2, 2, KINDS)),
                pltpu.SemaphoreType.DMA((2, 2, 2, KINDS)),
                pltpu.SemaphoreType.DMA((devices - 1,)),
                pltpu.SemaphoreType.DMA((devices - 1,)),
            ],
            compiler_params=pltpu.CompilerParams(collective_id=0, has_side_effects=True, vmem_limit_bytes=VMEM),
        )(*(pltpu.with_memory_space_constraint(x, pltpu.HBM) for x in (*map(blocks, terms), *map(blocks, weights), *m, *v)))
        new = store(new, VMEM)
        last = pl.pallas_call(
            functools.partial(gather_last, side),
            out_shape=here(wholes[2], jnp.bfloat16),
            in_specs=[pl.BlockSpec(memory_space=pltpu.HBM)],
            out_specs=pl.BlockSpec(memory_space=pltpu.VMEM),
            scratch_shapes=[*gather_sems, pltpu.SemaphoreType.DMA((2,))],
            compiler_params=pltpu.CompilerParams(collective_id=1, has_side_effects=True, vmem_limit_bytes=VMEM),
        )(pltpu.with_memory_space_constraint(new[2], pltpu.HBM))
        (last,) = store([last], VMEM)
        return (*(o.reshape(w.shape) for o, w in zip((*new[:2], last), weights, strict=True)), *new[3:])

    all_of, cut = P(None, None, None), P(None, "dp", None)
    return jax.shard_map(
        step,
        mesh=mesh,
        in_specs=(P(("rep", "dp"), None, None, None),) * 3 + (all_of,) * 3 + (cut,) * 6,
        out_specs=(P("rep", None, None),) * 3 + (P("rep", "dp", None),) * 6,
        check_vma=False,
    )
```

```python
import functools
import heapq
import math

import jax
import jax.numpy as jnp
from jax import lax
from jax.experimental import pallas as pl
from jax.experimental.pallas import tpu as pltpu
from jax.sharding import PartitionSpec as P

MESH = pl.DeviceIdType.MESH
F32 = jnp.float32
LEAD_NS = 23500
VMEM = 27 * 2**20
PARTS = (0, 1)
HALVES = (0, 1)
RINGS = 5
KINDS = 6


def gather_kinds(ring, fine):
    relays = {4: (1, 0, True), 5: (-1, 1, True)}
    if fine and ring == 3:
        return {0: (1, 0, False), 1: (-1, 1, False), 2: (1, 1, False), 3: (-1, 0, False), **relays}
    return {0: (1, None, False), 1: (-1, None, False), **relays}


def gather_order(slabs, fine):
    follow, waits = {}, {}
    for a, p in slabs:
        for ring in range(RINGS if fine else 2):
            for kind, (_, _, relayed) in gather_kinds(ring, fine).items():
                follow[a, p, ring, kind] = [(a, p, ring, 4 + kind)] if kind < 2 else []
        if fine:
            for kind, k in ((0, 3), (1, 1)):
                follow[a, p, 0, kind] += [(a, p, 1 + k, 0), (a, p, 1 + k, 1)]
            follow[a, p, 0, 4] += [(a, p, 3, 0), (a, p, 3, 3)]
            follow[a, p, 0, 5] += [(a, p, 3, 1), (a, p, 3, 2)]
        else:
            waits[a, p] = 4
    free, arrivals, order, made = {}, [], [], 0

    def put(send, now):
        nonlocal made
        a, p, ring, kind = send
        direction, half, _ = gather_kinds(ring, fine)[kind]
        way = (1 - p if ring == 0 else p, direction)
        time = (6.4 if half is None else 3.2) * (1 if fine or ring == 0 else 4)
        free[way] = max(now, free.get(way, 0.0)) + time
        made += 1
        heapq.heappush(arrivals, (free[way] + 2.0, made, send))

    for i, (a, p) in enumerate(slabs):
        for ring in (0, 1) if fine else (0,):
            for kind in (0, 1):
                put((a, p, ring, kind), 0.4 * i)
    while arrivals:
        now, _, send = heapq.heappop(arrivals)
        then = list(follow[send])
        if send[2] == 0 and not fine:
            waits[send[:2]] -= 1
            if waits[send[:2]] == 0:
                then += [(*send[:2], 1, 0), (*send[:2], 1, 1)]
        order.append((send, then))
        for one in then:
            put(one, now)
    return order


def moved(side, at, axis, by):
    return lax.rem(at[axis] + by + side, side)


def device(side, at, axis, by):
    to = moved(side, at, axis, by)
    return {"dp": to * side + at[1] if axis == 0 else at[0] * side + to}


def columns(wide, half):
    return pl.ds(half * (wide // 2), wide // 2)


def meet(side, at):
    barrier = pltpu.get_barrier_semaphore()
    for axis in (0, 1):
        for by in (1, -1):
            pl.semaphore_signal(barrier, inc=1, device_id=device(side, at, axis, by), device_id_type=MESH)
    pl.semaphore_wait(barrier, 4)


def gather_copy(side, at, whole, sems, fine, part, ring, kind, own=None):
    direction, half, relayed = gather_kinds(ring, fine)[kind]
    axis = 1 - part if ring == 0 else part
    along = moved(side, at, axis, -direction if relayed else 0)
    if ring == 1 and not fine:
        block = whole.at[part, along] if axis == 0 else whole.at[part, :, along]
        if half is not None:
            block = block.at[:, :, columns(whole.shape[-1], half)]
    else:
        other = at[1 - axis] if ring == 0 else moved(side, at, 1 - axis, ring - 1)
        block = whole.at[part, along, other] if axis == 0 else whole.at[part, other, along]
        if half is not None:
            block = block.at[:, columns(whole.shape[-1], half)]
    return pltpu.make_async_remote_copy(
        src_ref=own.at[part] if own is not None and ring < 2 and not relayed else block,
        dst_ref=block,
        send_sem=sems[0].at[part, ring, kind],
        recv_sem=sems[1].at[part, ring, kind],
        device_id=device(side, at, axis, direction),
        device_id_type=MESH,
    )


def sum_and_step(side, count, *refs):
    terms, weights, m_in, v_in = (refs[3 * i : 3 * i + 3] for i in range(4))
    fresh = refs[14]
    m_out, v_out, own, weight = (refs[15 + 3 * i : 18 + 3 * i] for i in range(4))
    slots = (*refs[12:14], refs[27])
    squares, load_sem, send_sem, recv_sem, gsend_sem, grecv_sem, nsend_sem, nrecv_sem = refs[28:]
    arrays = range(3)
    me = lax.axis_index("dp")
    at = (me // side, me % side)

    def place(axis, by):
        return moved(side, at, axis, by)

    def half_of(a, half):
        return columns(terms[a].shape[-1], half)

    def row_blocks(a):
        rows = terms[a].shape[-2]
        return 3 if rows % 48 == 0 else 1

    def load(a, p, which):
        if which == 0:
            t = place(p, 0)
            source = terms[a].at[0, p, t] if p == 0 else terms[a].at[0, p, :, t]
            return pltpu.make_async_copy(source, own[a].at[p, 0], load_sem.at[a, p, 0])
        half = which - 1
        t = place(p, 1 if half == 0 else -1)
        cols = half_of(a, half)
        source = terms[a].at[0, p, t, :, :, cols] if p == 0 else terms[a].at[0, p, :, t, :, cols]
        return pltpu.make_async_copy(source, own[a].at[p, 1, :, :, cols], load_sem.at[a, p, which])

    def load_state(a, which):
        if which == 0:
            return pltpu.make_async_copy(weights[a].at[:, at[0], at[1]], weight[a], load_sem.at[a, 0, 3])
        if which == 1:
            return pltpu.make_async_copy(m_in[a], m_out[a], load_sem.at[a, 1, 3])
        return pltpu.make_async_copy(v_in[a], v_out[a], load_sem.at[a, 0, 4])

    meet(side, at)
    pl.delay(lax.rem(lax.axis_index("rep"), 2) * LEAD_NS)

    def first(a, p, half, kind):
        up = 1 if half == 0 else -1
        cols = half_of(a, half)
        if kind == 2:
            source, by = own[a].at[p, 1, :, :, cols], up
        else:
            by = up if kind == 0 else -up
            t = place(p, 2 if kind == 0 else by)
            source = terms[a].at[0, p, t, :, :, cols] if p == 0 else terms[a].at[0, p, :, t, :, cols]
        return pltpu.make_async_remote_copy(
            src_ref=source,
            dst_ref=slots[a].at[p, kind, :, :, cols],
            send_sem=send_sem.at[a, p, half, kind],
            recv_sem=recv_sem.at[a, p, half, kind],
            device_id=device(side, at, p, by),
            device_id_type=MESH,
        )

    def second(a, p, half, kind):
        up = 1 if half == 0 else -1
        cols = half_of(a, half)
        by = -up if kind == 1 else up
        j = place(1 - p, 2 if kind == 0 else by)
        return pltpu.make_async_remote_copy(
            src_ref=own[a].at[p, 0, j, :, cols],
            dst_ref=slots[a].at[p, 3, kind, :, cols],
            send_sem=send_sem.at[a, p, half, 3 + kind],
            recv_sem=recv_sem.at[a, p, half, 3 + kind],
            device_id=device(side, at, 1 - p, by),
            device_id_type=MESH,
        )

    def rows_of(a, i):
        rows = terms[a].shape[-2] // row_blocks(a)
        return pl.ds(pl.multiple_of(i * rows, rows), rows)

    def add(a, p, half, j, extra):
        cols = half_of(a, half)

        def body(i, carry):
            rows = rows_of(a, i)
            total = own[a][p, 0, j, rows, cols].astype(F32)
            for k in (1, 2):
                total += slots[a][p, k, j, rows, cols].astype(F32)
            for k in extra:
                total += slots[a][p, 3, k, rows, cols].astype(F32)
            total = total.astype(jnp.bfloat16)
            own[a][p, 0, j, rows, cols] = total
            if carry is None:
                return None
            total = total.astype(F32)
            total = total * total
            total = sum(total[:, c : c + 128] for c in range(0, total.shape[1], 128))
            return carry + sum(total[r : r + 8] for r in range(0, total.shape[0], 8))

        return body

    every = [(p, half) for p in PARTS for half in HALVES]
    for a in arrays:
        for p, half in every:
            first(a, p, half, 0).start()
    for a in arrays:
        for p, half in every:
            load(a, p, 1 + half).start()
    for a in arrays:
        for p in PARTS:
            load(a, p, 0).start()
    for a in arrays:
        for which in range(3):
            load_state(a, which).start()
    for a in arrays:
        for p, half in every:
            first(a, p, half, 1).start()
            load(a, p, 1 + half).wait()
            first(a, p, half, 0).wait_recv()
            cols = half_of(a, half)
            blocks = row_blocks(a)

            def relay(i, _, a=a, p=p, cols=cols, blocks=blocks):
                j, rows = i // blocks, rows_of(a, i % blocks)
                total = own[a][p, 1, j, rows, cols].astype(F32) + slots[a][p, 0, j, rows, cols].astype(F32)
                own[a][p, 1, j, rows, cols] = total.astype(jnp.bfloat16)

            lax.fori_loop(0, side * blocks, relay, None)
            first(a, p, half, 2).start()
    for a in arrays:
        for p in PARTS:
            load(a, p, 0).wait()
        for p, half in every:
            up = 1 if half == 0 else -1
            first(a, p, half, 1).wait_recv()
            first(a, p, half, 2).wait_recv()
            for kind in (0, 1):
                j = place(1 - p, 2 if kind == 0 else -up)
                lax.fori_loop(0, row_blocks(a), lambda i, c, f=add(a, p, half, j, ()): f(i, c), None)
                second(a, p, half, kind).start()
    for a in arrays:
        for p, half in every:
            up = 1 if half == 0 else -1
            second(a, p, half, 0).wait_recv()
            lax.fori_loop(0, row_blocks(a), lambda i, c, f=add(a, p, half, place(1 - p, up), (0,)): f(i, c), None)
            second(a, p, half, 2).start()
    total = jnp.zeros((8, 128), F32)
    for a in arrays:
        for p, half in every:
            second(a, p, half, 1).wait_recv()
            second(a, p, half, 2).wait_recv()
            total = lax.fori_loop(0, row_blocks(a), add(a, p, half, at[1 - p], (1, 2)), total)

    def tell(axis, by):
        mine = squares.at[axis, at[axis]]
        return pltpu.make_async_remote_copy(
            src_ref=mine,
            dst_ref=mine,
            send_sem=nsend_sem.at[axis, by - 1],
            recv_sem=nrecv_sem.at[axis, by - 1],
            device_id=device(side, at, axis, by),
            device_id_type=MESH,
        )

    total = jnp.sum(total, axis=0, keepdims=True)
    for axis in (0, 1):
        squares[axis, at[axis]] = total
        for by in range(1, side):
            tell(axis, by).start()
        for by in range(1, side):
            tell(axis, by).wait_recv()
        total = squares[axis, 0]
        for i in range(1, side):
            total += squares[axis, i]
    for a in arrays:
        for which in range(3):
            load_state(a, which).wait()
        for p, half in every:
            for kind in range(3):
                first(a, p, half, kind).wait_send()
                second(a, p, half, kind).wait_send()
    total = jnp.sum(total, axis=1, keepdims=True)
    factor = jnp.minimum(1.0, 0.5 * lax.rsqrt(total / count + 1e-30))

    def send(a, *which):
        return gather_copy(side, at, slots[a], (gsend_sem.at[a], grecv_sem.at[a]), False, *which)

    for a in arrays:
        for p in PARTS:
            for half in HALVES:
                cols = half_of(a, half)

                def update(i, _, a=a, p=p, cols=cols):
                    rows = rows_of(a, i)
                    g = own[a][p, 0, at[1 - p], rows, cols].astype(F32) * factor
                    w = weight[a][p, rows, cols].astype(F32)
                    m = 0.9 * m_out[a][p, rows, cols] + 0.1 * g
                    v = 0.95 * v_out[a][p, rows, cols] + 0.05 * g * g
                    m_out[a][p, rows, cols] = m
                    v_out[a][p, rows, cols] = v
                    step = m * lax.rsqrt(v + 1e-8) + 0.1 * w
                    w = (w - 0.02 * step).astype(jnp.bfloat16)
                    if a == 2:
                        fresh[p, rows, cols] = w
                    else:
                        slots[a][p, at[0], at[1], rows, cols] = w

                lax.fori_loop(0, row_blocks(a), update, None)
            if a < 2:
                for kind in (0, 1):
                    send(a, p, 0, kind).start()
    slabs = [(a, p) for a in (0, 1) for p in PARTS]
    for one, then in gather_order(slabs, False):
        send(*one).wait_recv()
        for other in then:
            send(*other).start()
    for a, p in slabs:
        for ring in (0, 1):
            for kind in gather_kinds(ring, False):
                send(a, p, ring, kind).wait_send()
    for axis in (0, 1):
        for by in range(1, side):
            tell(axis, by).wait_send()


def gather_last(side, fresh, whole, send_sem, recv_sem, copy_sem):
    me = lax.axis_index("dp")
    at = (me // side, me % side)
    keep = [pltpu.make_async_copy(fresh.at[p], whole.at[p, at[0], at[1]], copy_sem.at[p]) for p in PARTS]
    for p in PARTS:
        keep[p].start()
    meet(side, at)

    def send(_, *which):
        return gather_copy(side, at, whole, (send_sem, recv_sem), True, *which, own=fresh)

    slabs = [(0, p) for p in PARTS]
    for a, p in slabs:
        for ring in (0, 1):
            for kind in (0, 1):
                send(a, p, ring, kind).start()
    for one, then in gather_order(slabs, True):
        send(*one).wait_recv()
        for other in then:
            send(*other).start()
    for p in PARTS:
        keep[p].wait()
        for ring in range(RINGS):
            for kind in gather_kinds(ring, True):
                send(0, p, ring, kind).wait_send()


def store(arrays, vmem):
    def body(*refs):
        here, there, sem = refs[: len(arrays)], refs[len(arrays) : -1], refs[-1]
        copies = [pltpu.make_async_copy(a, b, sem.at[i]) for i, (a, b) in enumerate(zip(here, there, strict=True))]
        for copy in copies:
            copy.start()
        for copy in copies:
            copy.wait()

    return pl.pallas_call(
        body,
        out_shape=[pltpu.HBM(x.shape, x.dtype) for x in arrays],
        in_specs=[pl.BlockSpec(memory_space=pltpu.VMEM)] * len(arrays),
        out_specs=[pl.BlockSpec(memory_space=pltpu.HBM)] * len(arrays),
        scratch_shapes=[pltpu.SemaphoreType.DMA((len(arrays),))],
        compiler_params=pltpu.CompilerParams(vmem_limit_bytes=vmem),
    )(*(pltpu.with_memory_space_constraint(x, pltpu.VMEM) for x in arrays))


def solution(mesh):
    devices = mesh.shape["dp"]
    side = math.isqrt(devices)

    def step(*arrays):
        terms, weights, m, v = (arrays[i : i + 3] for i in (0, 3, 6, 9))

        def blocks(x):
            return x.reshape(*x.shape[:-2], side, side, x.shape[-2] // devices, x.shape[-1])

        def here(shape, dtype):
            return pltpu.VMEM(shape, dtype)

        shapes = [one.shape for one in m]
        wholes = [blocks(w).shape for w in weights]
        count = devices * sum(math.prod(s) for s in shapes)
        gather_sems = [pltpu.SemaphoreType.DMA((2, RINGS, KINDS))] * 2
        new = pl.pallas_call(
            functools.partial(sum_and_step, side, count),
            out_shape=[here(s, jnp.bfloat16) for s in (*wholes[:2], shapes[2])] + [here(s, F32) for s in shapes * 2],
            in_specs=[pl.BlockSpec(memory_space=pltpu.HBM)] * 12,
            out_specs=[pl.BlockSpec(memory_space=pltpu.VMEM)] * 9,
            scratch_shapes=[pltpu.VMEM((2, 2, side, *s[1:]), jnp.bfloat16) for s in shapes]
            + [pltpu.VMEM(s, jnp.bfloat16) for s in (*shapes, wholes[2])]
            + [
                pltpu.VMEM((2, side, 1, 128), F32),
                pltpu.SemaphoreType.DMA((3, 2, 5)),
                pltpu.SemaphoreType.DMA((3, 2, 2, 6)),
                pltpu.SemaphoreType.DMA((3, 2, 2, 6)),
                pltpu.SemaphoreType.DMA((2, 2, 2, KINDS)),
                pltpu.SemaphoreType.DMA((2, 2, 2, KINDS)),
                pltpu.SemaphoreType.DMA((2, side - 1)),
                pltpu.SemaphoreType.DMA((2, side - 1)),
            ],
            compiler_params=pltpu.CompilerParams(collective_id=0, has_side_effects=True, vmem_limit_bytes=VMEM),
        )(*(pltpu.with_memory_space_constraint(x, pltpu.HBM) for x in (*map(blocks, terms), *map(blocks, weights), *m, *v)))
        new = store(new, VMEM)
        last = pl.pallas_call(
            functools.partial(gather_last, side),
            out_shape=here(wholes[2], jnp.bfloat16),
            in_specs=[pl.BlockSpec(memory_space=pltpu.HBM)],
            out_specs=pl.BlockSpec(memory_space=pltpu.VMEM),
            scratch_shapes=[*gather_sems, pltpu.SemaphoreType.DMA((2,))],
            compiler_params=pltpu.CompilerParams(collective_id=1, has_side_effects=True, vmem_limit_bytes=VMEM),
        )(pltpu.with_memory_space_constraint(new[2], pltpu.HBM))
        (last,) = store([last], VMEM)
        return (*(o.reshape(w.shape) for o, w in zip((*new[:2], last), weights, strict=True)), *new[3:])

    all_of, cut = P(None, None, None), P(None, "dp", None)
    return jax.shard_map(
        step,
        mesh=mesh,
        in_specs=(P(("rep", "dp"), None, None, None),) * 3 + (all_of,) * 3 + (cut,) * 6,
        out_specs=(P("rep", None, None),) * 3 + (P("rep", "dp", None),) * 6,
        check_vma=False,
    )
```
